32 devices in a mesh: cfg: 2 (over y), seq: 8 (over z, core), tp: 2 (over x).
Axes of the slice: x: 2, y: 2, z: 4, core: 2. Of those that a mesh axis runs over, the one named last changes fastest.
Arguments:
- queries: bfloat16 [2, 3840, 5120], P('cfg', 'seq', 'tp'), may hold values from -5 to 5
- keys: bfloat16 [2, 3840, 5120], P('cfg', 'seq', 'tp'), may hold values from -5 to 5
- values: bfloat16 [2, 3840, 5120], P('cfg', 'seq', 'tp'), may hold values from -5 to 5
- text_keys: bfloat16 [2, 512, 5120], P('cfg', None, 'tp'), may hold values from -7.5 to 7.5
- text_values: bfloat16 [2, 512, 5120], P('cfg', None, 'tp'), may hold values from -5 to 5
- prompt_lengths: int32 [2], P('cfg'), may hold values from 64 to 512
- frame_counts: int32 [8], P('seq'), may hold values from 240 to 480
- out_weight: bfloat16 [5120, 5120], P('tp'), may hold values from -0.5 to 0.5
Outputs:
- velocity: bfloat16 [3840, 5120], P('seq', ('tp', 'cfg'))
The draws below stay inside these ranges and needn't reach their ends.
All inputs are finite; a program needn't handle non-finite values.
Results may differ from the reference program's by a relative error of at most 0.015.
Values may be sent and summed in bfloat16 or wider, within the bound.
A program may use at most 320 MiB of HBM per device.

```python
import jax
import jax.numpy as jnp
from jax import lax

HEADS = 40
HEAD_DIM = 128
D = 5120
TEXT = 512
FRAME_SLOTS = 480
FRAMES = 8
TOKENS = 3840


def query_key_pair(key):
    base = jax.random.fold_in(key, 7)
    shape = (2, TOKENS, D)
    query_draw = jnp.clip(1.5 * jax.random.normal(jax.random.fold_in(base, 1), shape, jnp.float32), -5.0, 5.0)
    key_draw = jnp.clip(jax.random.normal(jax.random.fold_in(base, 2), shape, jnp.float32), -5.0, 5.0)
    return (query_draw, key_draw)


def draw_queries(key, part):
    return query_key_pair(key)[0].astype(jnp.bfloat16)


def draw_keys(key, part):
    return query_key_pair(key)[1].astype(jnp.bfloat16)


def touch_ends(entries, key, least, top_value):
    longest = entries.shape.index(max(entries.shape))
    spots = []
    for shift in (0, 1):
        where = [jax.random.randint(jax.random.fold_in(key, axis), (), 0, length) for axis, length in enumerate(entries.shape)]
        where[longest] = (where[longest] + shift) % entries.shape[longest]
        spots.append(tuple(where))
    return entries.at[spots[0]].set(least).at[spots[1]].set(top_value)


def levels(rng, shape, shards, smallest, high):
    def one(position, blocks):
        draws = jax.random.uniform(jax.random.fold_in(jax.random.fold_in(rng, 6), position), (blocks,), jnp.float32, smallest / len(shards), high / len(shards))
        return jnp.repeat(jnp.exp(draws), shape[position] // blocks).reshape((-1,) + (1,) * (len(shape) - position - 1))

    gain = one(*shards[0])
    for cut in shards[1:]:
        gain = gain * one(*cut)
    return gain


def normal_values(stream_key, extent, scale, limit, shards=(), kind=jnp.bfloat16):
    level = levels(stream_key, extent, shards, -0.22, 0.18) if shards else 1.0
    array = jax.random.normal(stream_key, extent, jnp.float32) * scale * level
    return jnp.minimum(jnp.maximum(array, -limit), limit).astype(kind)


def setup_inputs(seed: int = 0) -> dict:
    seeds = jax.random.split(jax.random.key(seed), 9)
    return {
        "queries": draw_queries(jax.random.fold_in(seeds[8], 71), 0),
        "keys": draw_keys(jax.random.fold_in(seeds[8], 71), 0),
        "values": normal_values(seeds[2], (2, TOKENS, D), 1.0, 5.0, ((0, 2), (1, 8), (2, 2))),
        "text_keys": normal_values(seeds[3], (2, TEXT, D), 1.5, 7.5, ((0, 2), (2, 2))),
        "text_values": normal_values(seeds[4], (2, TEXT, D), 1.0, 5.0, ((0, 2), (2, 2))),
        "prompt_lengths": jax.random.randint(seeds[5], (2,), TEXT // 8, TEXT + 1).astype(jnp.int32),
        "frame_counts": touch_ends(jax.random.randint(seeds[6], (FRAMES,), FRAME_SLOTS // 2, FRAME_SLOTS + 1), jax.random.fold_in(seeds[6], 1), FRAME_SLOTS // 2, FRAME_SLOTS).astype(jnp.int32),
        "out_weight": normal_values(seeds[7], (D, D), (D // 32) ** -0.5, 0.5, ((0, 2),)),
    }


GUIDANCE = 5.0
RESCALE = 0.7
NEGATIVE = -1e+30

def video_valid(frame_counts):
    positions = jnp.arange(TOKENS, dtype=jnp.int32)
    return positions % FRAME_SLOTS < frame_counts[positions // FRAME_SLOTS]

def branch_output(query_rows, key_rows, value_rows, text_key_rows, text_value_rows, length, video_mask, out_weight):
    text_mask = jnp.arange(TEXT, dtype=jnp.int32) < length
    full_mask = jnp.concatenate([text_mask, video_mask])
    all_keys = jnp.concatenate([text_key_rows, key_rows], axis=0)
    all_values = jnp.concatenate([text_value_rows, value_rows], axis=0)
    key_total = all_keys.shape[0]
    query_heads = jnp.transpose(query_rows.reshape(TOKENS, HEADS, HEAD_DIM), (1, 0, 2))
    key_heads = jnp.transpose(all_keys.reshape(key_total, HEADS, HEAD_DIM), (1, 0, 2))
    value_heads = jnp.transpose(all_values.reshape(key_total, HEADS, HEAD_DIM), (1, 0, 2))

    def one_head(operands):
        query_head, key_head, value_head = operands
        scores = jnp.dot(query_head, key_head.T, preferred_element_type=jnp.float32) * HEAD_DIM ** (-0.5)
        scores = jnp.where(full_mask[None, :], scores, NEGATIVE)
        row_max = lax.optimization_barrier(jnp.max(scores, axis=1, keepdims=True))
        weights = jnp.exp(scores - row_max)
        weight_sum = lax.optimization_barrier(jnp.sum(weights, axis=1, keepdims=True))
        mixed_rows = jnp.dot(weights.astype(jnp.bfloat16), value_head, preferred_element_type=jnp.float32)
        return (mixed_rows / weight_sum).astype(jnp.bfloat16)
    heads_out = lax.map(one_head, (query_heads, key_heads, value_heads))
    attended = jnp.transpose(heads_out, (1, 0, 2)).reshape(TOKENS, HEADS * HEAD_DIM)
    return jnp.dot(attended, out_weight, preferred_element_type=jnp.float32).astype(jnp.bfloat16)

def reference(queries, keys, values, text_keys, text_values, prompt_lengths, frame_counts, out_weight):
    video_mask = video_valid(frame_counts)
    conditional = branch_output(queries[0], keys[0], values[0], text_keys[0], text_values[0], prompt_lengths[0], video_mask, out_weight).astype(jnp.float32)
    unconditional = branch_output(queries[1], keys[1], values[1], text_keys[1], text_values[1], prompt_lengths[1], video_mask, out_weight).astype(jnp.float32)
    guided = unconditional + GUIDANCE * (conditional - unconditional)
    token_weights = video_mask.astype(jnp.float32)
    valid_total = jnp.sum(frame_counts).astype(jnp.float32)

    def moment(field_rows):
        return jnp.dot(token_weights, field_rows, precision=lax.Precision.HIGHEST) / valid_total
    guided_mean = moment(guided)
    guided_var = moment(guided * guided) - guided_mean * guided_mean
    cond_mean = moment(conditional)
    cond_var = moment(conditional * conditional) - cond_mean * cond_mean
    std_ratio = jnp.sqrt((cond_var + 1.0) / (guided_var + 1.0))
    factor = RESCALE * std_ratio + (1.0 - RESCALE)
    return (guided_mean + (guided - guided_mean) * factor).astype(jnp.bfloat16)
```

```python
import functools

import jax
import jax.numpy as jnp
from jax import lax
from jax.experimental import pallas as pl
from jax.experimental.pallas import tpu as pltpu
from jax.sharding import PartitionSpec as P

HEAD_DIM = 128
GUIDANCE = 5.0
RESCALE = 0.7
NEGATIVE = -1e30
LOG2E = 1.4426950408889634
CORES = 2
MESH = pl.DeviceIdType.MESH


def chunk_rows(total, limit):
    for unit in (256, 128, 16):
        for size in range(limit // unit * unit, 0, -unit):
            if total % size == 0:
                return size
    return total


def step_kernel(
    n, chips, group, rows, text, wide,
    q, k, v, tk, tv, w, counts, lengths,
    out,
    qb, kb, vb, tkb, tvb, cb, bias, tbias, ob, ab, wb, acc, st, sg,
    send, recv, fsend, frecv, csend, crecv, local, tlocal, osend, orecv,
    xsend, xrecv, ysend, yrecv, rsend, rrecv,
    wlocal, wsend, wrecv, wfsend, wfrecv, ssend, srecv,
):
    me = lax.axis_index("seq")
    t = lax.axis_index("tp")
    c = lax.axis_index("cfg")
    core = lax.rem(me, CORES)
    chip = lax.div(me, CORES)
    partner = chip * CORES + (CORES - 1 - core)
    scale = LOG2E * HEAD_DIM ** (-0.5)
    last = group - 1
    half = chips // 2
    bf16 = jnp.bfloat16
    f32 = jnp.float32

    def cols(owner, head):
        return pl.ds(pl.multiple_of((owner * group + head) * HEAD_DIM, HEAD_DIM), HEAD_DIM)

    def out_cols(side, branch):
        return pl.ds(pl.multiple_of((side * 2 + branch) * wide, HEAD_DIM), wide)

    def slot(index):
        return pl.ds(pl.multiple_of(index * rows, 16), rows)

    def chip_at(step):
        return lax.rem(chip + step, chips)

    def chip_back(step):
        return lax.rem(chip + chips - step, chips)

    def across(src, dst, sends, recvs, device):
        return pltpu.make_async_remote_copy(
            src_ref=src, dst_ref=dst, send_sem=sends, recv_sem=recvs,
            device_id=device, device_id_type=MESH,
        )

    x_side = {"tp": 1 - t}
    y_side = {"cfg": 1 - c}

    def kv_copies(head, step):
        target = chip_at(step)
        return [
            across(
                src.at[:, cols(target, head)], dst.at[head, slot(me)],
                send.at[index, head, step - 1], recv.at[index, head, step - 1],
                {"seq": target * CORES + core},
            )
            for index, (src, dst) in enumerate(((k, kb), (v, vb)))
        ]

    def q_copy(head, step):
        target = chip_at(step)
        return across(
            q.at[:, cols(target, head)], qb.at[head, chip],
            send.at[2, head, step - 1], recv.at[2, head, step - 1],
            {"seq": target * CORES + core},
        )

    def own_copies(head):
        return [
            pltpu.make_async_copy(k.at[:, cols(chip, head)], kb.at[head, slot(me)], local.at[0, head]),
            pltpu.make_async_copy(v.at[:, cols(chip, head)], vb.at[head, slot(me)], local.at[1, head]),
            pltpu.make_async_copy(q.at[:, cols(chip, head)], qb.at[head, chip], local.at[2, head]),
            pltpu.make_async_copy(tk.at[:, cols(chip, head)], tkb.at[head], tlocal.at[0, head]),
            pltpu.make_async_copy(tv.at[:, cols(chip, head)], tvb.at[head], tlocal.at[1, head]),
        ]

    def own_forward(head):
        return [
            across(
                src.at[:, cols(chip, head)], dst.at[head, slot(me)],
                fsend.at[index, head, 0], frecv.at[index, head, 0], {"seq": partner},
            )
            for index, (src, dst) in enumerate(((k, kb), (v, vb)))
        ]

    def forward(index, head, step):
        place = (kb, vb)[index].at[head, slot(chip_back(step) * CORES + core)]
        return across(
            place, place, fsend.at[index, head, step], frecv.at[index, head, step],
            {"seq": partner},
        )

    def count_copy(step):
        return across(
            counts, cb.at[me], csend.at[step - 1], crecv.at[step - 1],
            {"seq": lax.rem(me + step, n)},
        )

    def out_copy(head, step):
        target = chip_at(step)
        return across(
            ob.at[head, target], ab.at[c, t, head, chip],
            osend.at[head, step], orecv.at[head, step], {"seq": target * CORES + core},
        )

    def own_out(head):
        return pltpu.make_async_copy(
            ob.at[head, chip], ab.at[c, t, head, chip], orecv.at[head, 0]
        )

    def x_copy(head, index):
        place = ab.at[c, t, head, chip_back(index)]
        return across(place, place, xsend.at[head, index], xrecv.at[head, index], x_side)

    def y_copy(head, index):
        place = ab.at[c, t, head, chip_back(index)]
        return across(place, place, ysend.at[head, index], yrecv.at[head, index], y_side)

    def relay(head, index):
        if index % 2 == 0:
            place = ab.at[1 - c, t, head, chip_back(index)]
            side = x_side
        else:
            place = ab.at[c, 1 - t, head, chip_back(index)]
            side = y_side
        return across(place, place, rsend.at[head, index], rrecv.at[head, index], side)

    def w_own(head):
        return pltpu.make_async_copy(
            w.at[:, head, :, out_cols(t, c)], wb.at[head, t], wlocal.at[head]
        )

    def w_copy(head):
        part = pl.ds(core * half, half)
        return across(
            w.at[part, head, :, out_cols(1 - t, c)], wb.at[head, t, part],
            wsend.at[head], wrecv.at[head], x_side,
        )

    def w_forward(head):
        place = wb.at[head, 1 - t, pl.ds(core * half, half)]
        return across(place, place, wfsend.at[head], wfrecv.at[head], {"seq": partner})

    def stat_copy(step):
        return across(
            st, sg.at[me], ssend.at[step - 1], srecv.at[step - 1],
            {"seq": lax.rem(me + step, n)},
        )

    barrier = pltpu.get_barrier_semaphore()
    for step in range(1, n):
        pl.semaphore_signal(
            barrier, inc=1, device_id={"seq": lax.rem(me + step, n)}, device_id_type=MESH
        )
    pl.semaphore_signal(barrier, inc=1, device_id=x_side, device_id_type=MESH)
    pl.semaphore_signal(barrier, inc=1, device_id=y_side, device_id_type=MESH)

    def start_own(head, _):
        for copy in own_copies(head):
            copy.start()
        w_own(head).start()
        return 0

    lax.fori_loop(0, group, start_own, 0)
    pl.semaphore_wait(barrier, n + 1)

    def start_kv(head):
        for step in range(1, chips):
            for copy in kv_copies(head, step):
                copy.start()

    def start_q(head):
        for step in range(1, chips):
            q_copy(head, step).start()

    def start_first(head, _):
        start_kv(head)
        start_q(head)
        return 0

    for step in range(1, n):
        count_copy(step).start()
    lax.fori_loop(0, 2, start_first, 0)

    def start_near(head, _):
        w_copy(head).start()
        for copy in own_forward(head):
            copy.start()
        return 0

    lax.fori_loop(0, group, start_near, 0)

    cb[me] = counts[...]
    st[...] = jnp.zeros_like(st)
    for step in range(1, n):
        count_copy(step).wait_recv()
    lane = lax.broadcasted_iota(jnp.int32, (rows, HEAD_DIM), 1)
    place_in = lax.broadcasted_iota(jnp.int32, (rows, HEAD_DIM), 0)

    def fill_bias(source, _):
        limit = cb[source][0:1, :]
        bias[slot(source), :] = jnp.where(
            (lane == 0) & (place_in >= limit), NEGATIVE, 0.0
        ).astype(bf16)
        return 0

    lax.fori_loop(0, n, fill_bias, 0)
    tlane = lax.broadcasted_iota(jnp.int32, (text, HEAD_DIM), 1)
    tplace = lax.broadcasted_iota(jnp.int32, (text, HEAD_DIM), 0)
    tbias[...] = jnp.where(
        (tlane == 0) & (tplace >= lengths[0:1, :]), NEGATIVE, 0.0
    ).astype(bf16)

    total = n * rows
    size = chunk_rows(total, 768)

    def ones(length):
        return jnp.where(
            lax.broadcasted_iota(jnp.int32, (length, HEAD_DIM), 1) == 0, 1.0, 0.0
        ).astype(bf16)

    def one_block(head, target):
        query = jnp.concatenate([qb[head, target], ones(rows)], axis=1)

        def piece(state, keys, masks, vals):
            keys = jnp.concatenate([keys, masks], axis=1)
            vals = jnp.concatenate([vals, ones(vals.shape[0])], axis=1)
            scores = lax.dot_general(
                query, keys, (((1,), (1,)), ((), ())), preferred_element_type=f32
            )
            high = jnp.max(scores, axis=1, keepdims=True) * scale
            if state is not None:
                high = jnp.maximum(high, state[0])
            weights = jnp.exp2(scores * scale - high).astype(bf16)
            mixed = jnp.dot(weights, vals, preferred_element_type=f32)
            if state is not None:
                mixed = mixed + state[1] * jnp.exp2(state[0] - high)
            return (high, mixed)

        state = piece(None, tkb[head], tbias[...], tvb[head])
        for start in range(0, total, size):
            span = pl.ds(start, size)
            state = piece(state, kb[head, span], bias[span, :], vb[head, span])
        mixed = state[1]
        ob[head, target] = (
            mixed[:, :HEAD_DIM] / mixed[:, HEAD_DIM:HEAD_DIM + 1]
        ).astype(bf16)

    def take_keys(head):
        for copy in own_copies(head):
            copy.wait()
        for step in range(1, chips):
            made = kv_copies(head, step)
            for index in range(2):
                made[index].wait_recv()
                forward(index, head, step).start()
        for copy in own_forward(head):
            copy.wait_recv()
        for step in range(1, chips):
            for index in range(2):
                forward(index, head, step).wait_recv()

    def blocks(head, between):
        def block(step, _):
            far = step < chips

            @pl.when(far)
            def _():
                q_copy(head, step).wait_recv()

            one_block(head, chip_back(step))

            @pl.when(far)
            def _():
                out_copy(head, chips - step).start()

            @pl.when(step == chips)
            def _():
                own_out(head).start()

            if between is not None:
                @pl.when(step == 2)
                def _():
                    between()
            return 0

        lax.fori_loop(1, chips + 1, block, 0)

    def share(head):
        for index in (0, *range(chips - 1, 0, -1)):
            if index == 0:
                own_out(head).wait()
            else:
                out_copy(head, index).wait_recv()
            x_copy(head, index).start()
            y_copy(head, index).start()

    def pass_on(head):
        for index in (0, *range(chips - 1, 0, -1)):
            (x_copy if index % 2 else y_copy)(head, index).wait_recv()
            relay(head, index).start()

    def collect(head):
        for index in range(chips):
            (y_copy if index % 2 else x_copy)(head, index).wait_recv()
        for index in range(chips):
            relay(head, index).wait_recv()
        w_own(head).wait()
        w_forward(head).wait_recv()

    part = 256 if wide % 256 == 0 else HEAD_DIM
    depth = CORES * chips * HEAD_DIM

    def product(head, branch, span):
        rows_in = jnp.concatenate(
            [ab[branch, side, head, source] for side in range(2) for source in range(chips)],
            axis=1,
        )
        weight = wb[head, :, :, :, span].reshape(depth, part)
        return jnp.dot(rows_in, weight, preferred_element_type=f32)

    def span_of(index):
        return pl.ds(pl.multiple_of(index * part, HEAD_DIM), part)

    def project(head):
        def one(index, _):
            span = span_of(index)
            for branch in range(2):
                acc[branch, :, span] += product(head, branch, span)
            return 0

        lax.fori_loop(0, wide // part, one, 0)

    acc[...] = jnp.zeros_like(acc)

    def one_head(head, _):
        take_keys(head)
        blocks(head, None)

        @pl.when(head + 2 < group)
        def _():
            start_kv(head + 2)

        @pl.when(head + 2 < last)
        def _():
            start_q(head + 2)

        @pl.when(head + 1 == last)
        def _():
            start_q(last)

        @pl.when(head == 1)
        def _():
            def pass_weight(index, _):
                w_copy(index).wait_recv()
                w_forward(index).start()
                return 0

            lax.fori_loop(0, group, pass_weight, 0)

        @pl.when(head >= 1)
        def _():
            share(head - 1)
            pass_on(head - 1)
            collect(head - 1)
            project(head - 1)

        return 0

    lax.fori_loop(0, last, one_head, 0)
    take_keys(last)
    share(last - 1)
    blocks(last, lambda: pass_on(last - 1))
    share(last)
    collect(last - 1)
    project(last - 1)
    pass_on(last)
    collect(last)

    limit = counts[0:1, 0:1]
    valid = lax.broadcasted_iota(jnp.int32, (rows, part), 0) < limit

    def guide(index, _):
        span = span_of(index)
        conditional, unconditional = [
            (acc[branch, :, span] + product(last, branch, span)).astype(bf16).astype(f32)
            for branch in range(2)
        ]
        guided = unconditional + GUIDANCE * (conditional - unconditional)
        acc[0, :, span] = guided
        guided = jnp.where(valid, guided, 0.0)
        conditional = jnp.where(valid, conditional, 0.0)
        for row, field in enumerate(
            (guided, guided * guided, conditional, conditional * conditional)
        ):
            st[row:row + 1, span] = jnp.sum(field, axis=0, keepdims=True)
        st[4:5, span] = jnp.broadcast_to(limit.astype(f32), (1, part))
        return 0

    lax.fori_loop(0, wide // part, guide, 0)

    for step in range(1, n):
        stat_copy(step).start()
    sg[me] = st[...]

    def settle(head, _):
        for step in range(1, chips):
            for copy in kv_copies(head, step):
                copy.wait_send()
            q_copy(head, step).wait_send()
            out_copy(head, step).wait_send()
            for index in range(2):
                forward(index, head, step).wait_send()
        for copy in own_forward(head):
            copy.wait_send()
        for index in range(chips):
            x_copy(head, index).wait_send()
            y_copy(head, index).wait_send()
            relay(head, index).wait_send()
        w_copy(head).wait_send()
        w_forward(head).wait_send()
        return 0

    lax.fori_loop(0, group, settle, 0)
    for step in range(1, n):
        count_copy(step).wait_send()
    for step in range(1, n):
        stat_copy(step).wait()
    sums = sg[0]
    for source in range(1, n):
        sums = sums + sg[source]
    st[...] = sums

    def finish(index, _):
        span = span_of(index)
        here = st[:, span]
        valid_total = here[4:5, :]
        guided_mean = here[0:1, :] / valid_total
        guided_var = here[1:2, :] / valid_total - guided_mean * guided_mean
        cond_mean = here[2:3, :] / valid_total
        cond_var = here[3:4, :] / valid_total - cond_mean * cond_mean
        std_ratio = jnp.sqrt((cond_var + 1.0) / (guided_var + 1.0))
        factor = RESCALE * std_ratio + (1.0 - RESCALE)
        out[:, span] = (guided_mean + (acc[0, :, span] - guided_mean) * factor).astype(bf16)
        return 0

    lax.fori_loop(0, wide // part, finish, 0)


def fused_step(
    queries, keys, values, text_keys, text_values, prompt_lengths, frame_counts, out_weight, n
):
    rows, width = queries.shape
    text = text_keys.shape[0]
    chips = n // CORES
    heads = width // HEAD_DIM
    group = heads // chips
    wide = out_weight.shape[1] // 4
    counts = jnp.broadcast_to(frame_counts.reshape(1, 1), (8, HEAD_DIM))
    lengths = jnp.broadcast_to(prompt_lengths.reshape(1, 1), (8, HEAD_DIM))
    weight = out_weight.reshape(chips, group, HEAD_DIM, out_weight.shape[1])
    bf16 = jnp.bfloat16
    f32 = jnp.float32
    total = n * rows
    hbm = pl.BlockSpec(memory_space=pl.ANY)
    vmem = pl.BlockSpec(memory_space=pltpu.VMEM)
    dma = pltpu.SemaphoreType.DMA
    return pl.pallas_call(
        functools.partial(step_kernel, n, chips, group, rows, text, wide),
        out_shape=jax.ShapeDtypeStruct((rows, wide), bf16),
        in_specs=[hbm] * 6 + [vmem] * 2,
        out_specs=vmem,
        scratch_shapes=[
            pltpu.VMEM((group, chips, rows, HEAD_DIM), bf16),
            pltpu.VMEM((group, total, HEAD_DIM), bf16),
            pltpu.VMEM((group, total, HEAD_DIM), bf16),
            pltpu.VMEM((group, text, HEAD_DIM), bf16),
            pltpu.VMEM((group, text, HEAD_DIM), bf16),
            pltpu.VMEM((n, 8, HEAD_DIM), jnp.int32),
            pltpu.VMEM((total, HEAD_DIM), bf16),
            pltpu.VMEM((text, HEAD_DIM), bf16),
            pltpu.VMEM((group, chips, rows, HEAD_DIM), bf16),
            pltpu.VMEM((2, 2, group, chips, rows, HEAD_DIM), bf16),
            pltpu.VMEM((group, 2, chips, HEAD_DIM, wide), bf16),
            pltpu.VMEM((2, rows, wide), f32),
            pltpu.VMEM((8, wide), f32),
            pltpu.VMEM((n, 8, wide), f32),
            dma((3, group, chips - 1)),
            dma((3, group, chips - 1)),
            dma((2, group, chips)),
            dma((2, group, chips)),
            dma((n - 1,)),
            dma((n - 1,)),
            dma((3, group)),
            dma((2, group)),
            dma((group, chips)),
            dma((group, chips)),
            dma((group, chips)),
            dma((group, chips)),
            dma((group, chips)),
            dma((group, chips)),
            dma((group, chips)),
            dma((group, chips)),
            dma((group,)),
            dma((group,)),
            dma((group,)),
            dma((group,)),
            dma((group,)),
            dma((n - 1,)),
            dma((n - 1,)),
        ],
        compiler_params=pltpu.CompilerParams(
            collective_id=0, has_side_effects=True, vmem_limit_bytes=62 * 1024 * 1024
        ),
    )(queries, keys, values, text_keys, text_values, weight, counts, lengths)


def frame_valid(positions, counts_table, slots):
    frame_index = positions // slots
    slot_index = positions % slots
    frame_ids = jnp.arange(counts_table.shape[0], dtype=jnp.int32)
    frame_limit = jnp.sum(
        jnp.where(frame_index[:, None] == frame_ids[None, :], counts_table[None, :], 0), axis=1
    )
    return slot_index < frame_limit


def attend_block(carry, key_rows, value_rows, query_heads, key_mask):
    row_max, weight_sum, mixed_sum = carry
    head_count = query_heads.shape[1]
    key_heads = key_rows.reshape(key_rows.shape[0], head_count, HEAD_DIM)
    value_heads = value_rows.reshape(value_rows.shape[0], head_count, HEAD_DIM)
    scores = jnp.einsum(
        "qhd,khd->hqk", query_heads, key_heads, preferred_element_type=jnp.float32
    ) * HEAD_DIM ** (-0.5)
    scores = jnp.where(key_mask[None, None, :], scores, NEGATIVE)
    new_max = jnp.maximum(row_max, jnp.max(scores, axis=2))
    shrink = jnp.exp(row_max - new_max)
    weights = jnp.exp(scores - new_max[:, :, None])
    weight_sum = weight_sum * shrink + jnp.sum(weights, axis=2)
    mixed_sum = mixed_sum * shrink[:, :, None] + jnp.einsum(
        "hqk,khd->hqd",
        weights.astype(jnp.bfloat16),
        value_heads,
        preferred_element_type=jnp.float32,
    )
    return (new_max, weight_sum, mixed_sum)


def gathered_attention(
    queries, keys, values, text_keys, text_values, prompt_lengths, frame_counts, n
):
    row_count, head_cols = queries.shape
    head_count = head_cols // HEAD_DIM
    all_counts = lax.all_gather(frame_counts, "seq", axis=0, tiled=True)
    query_heads = queries.reshape(row_count, head_count, HEAD_DIM)
    text_mask = jnp.arange(text_keys.shape[0], dtype=jnp.int32) < prompt_lengths[0]
    empty_state = (
        jnp.full((head_count, row_count), NEGATIVE, jnp.float32),
        jnp.zeros((head_count, row_count), jnp.float32),
        jnp.zeros((head_count, row_count, HEAD_DIM), jnp.float32),
    )
    text_state = attend_block(empty_state, text_keys, text_values, query_heads, text_mask)
    key_rows = lax.all_gather(keys, "seq", axis=0, tiled=True)
    value_rows = lax.all_gather(values, "seq", axis=0, tiled=True)
    positions = jnp.arange(key_rows.shape[0], dtype=jnp.int32)
    _, weight_sum, mixed_sum = attend_block(
        text_state, key_rows, value_rows, query_heads,
        frame_valid(positions, all_counts, row_count // frame_counts.shape[0]),
    )
    return (
        jnp.transpose(mixed_sum / weight_sum[:, :, None], (1, 0, 2))
        .reshape(row_count, head_cols)
        .astype(jnp.bfloat16)
    )


def fits_fused(n, cfgs, tps, queries, frame_counts, out_weight):
    heads = queries.shape[2] // HEAD_DIM
    chips = n // CORES
    if cfgs != 2 or tps != 2 or n % CORES or frame_counts.shape[0] != 1:
        return False
    if chips < 2 or chips % 2 or heads % chips or heads // chips < 3:
        return False
    return out_weight.shape[1] % (4 * HEAD_DIM) == 0 and queries.shape[1] % 16 == 0


def body(n, cfgs, tps, queries, keys, values, text_keys, text_values, prompt_lengths, frame_counts, out_weight):
    rows = queries.shape[1]
    if fits_fused(n, cfgs, tps, queries, frame_counts, out_weight):
        return fused_step(
            queries[0], keys[0], values[0], text_keys[0], text_values[0],
            prompt_lengths, frame_counts, out_weight, n,
        )
    attended = gathered_attention(
        queries[0], keys[0], values[0], text_keys[0], text_values[0],
        prompt_lengths, frame_counts, n,
    )
    branch = lax.psum_scatter(
        lax.dot_general(
            out_weight, attended, (((0,), (1,)), ((), ())), preferred_element_type=jnp.float32
        ).astype(jnp.bfloat16),
        "tp",
        scatter_dimension=0,
        tiled=True,
    )
    half = branch.shape[0] // cfgs
    mine = lax.axis_index("cfg")
    kept = lax.dynamic_slice_in_dim(branch, mine * half, half, 0)
    given = lax.dynamic_slice_in_dim(branch, (1 - mine) * half, half, 0)
    other = lax.ppermute(given, "cfg", [(0, 1), (1, 0)])
    first = mine == 0
    conditional = jnp.where(first, kept, other).astype(jnp.float32)
    unconditional = jnp.where(first, other, kept).astype(jnp.float32)
    guided = unconditional + GUIDANCE * (conditional - unconditional)
    valid = (jnp.arange(rows, dtype=jnp.int32) < frame_counts[0])[None, :]

    def local_sum(field):
        return jnp.sum(jnp.where(valid, field, 0.0), axis=1)

    sums = lax.psum(
        jnp.stack([
            local_sum(guided),
            local_sum(guided * guided),
            local_sum(conditional),
            local_sum(conditional * conditional),
            jnp.full((half,), frame_counts[0].astype(jnp.float32)),
        ]),
        "seq",
    )
    means = sums[:4] / sums[4:5]
    guided_mean = means[0]
    guided_var = means[1] - guided_mean * guided_mean
    cond_var = means[3] - means[2] * means[2]
    std_ratio = jnp.sqrt((cond_var + 1.0) / (guided_var + 1.0))
    factor = RESCALE * std_ratio + (1.0 - RESCALE)
    velocity = guided_mean[:, None] + (guided - guided_mean[:, None]) * factor[:, None]
    return velocity.astype(jnp.bfloat16).T


def solution(mesh):
    placed = (
        P("cfg", "seq", "tp"),
        P("cfg", "seq", "tp"),
        P("cfg", "seq", "tp"),
        P("cfg", None, "tp"),
        P("cfg", None, "tp"),
        P("cfg"),
        P("seq"),
        P("tp", None),
    )
    return jax.shard_map(
        functools.partial(body, mesh.shape["seq"], mesh.shape["cfg"], mesh.shape["tp"]),
        mesh=mesh, in_specs=placed, out_specs=P("seq", ("tp", "cfg")), check_vma=False,
    )
```

```python
import functools

import jax
import jax.numpy as jnp
from jax import lax
from jax.experimental import pallas as pl
from jax.experimental.pallas import tpu as pltpu
from jax.sharding import PartitionSpec as P

HEAD_DIM = 128
GUIDANCE = 5.0
RESCALE = 0.7
NEGATIVE = -1e30
LOG2E = 1.4426950408889634
CORES = 2
MESH = pl.DeviceIdType.MESH


def chunk_rows(total, limit):
    for unit in (256, 128, 16):
        for size in range(limit // unit * unit, 0, -unit):
            if total % size == 0:
                return size
    return total


def step_kernel(
    n, chips, group, rows, text, wide, part,
    q, k, v, tk, tv, w, counts, lengths,
    out,
    qb, kb, vb, tkb, tvb, mc, cb, bias, tbias, ob, ab, wb, acc, st, sg, vel,
    send, krecv, qrecv, frecv, count, local, orecv, passed, direct, relayed, wsem, stat, vsem,
):
    me = lax.axis_index("seq")
    t = lax.axis_index("tp")
    c = lax.axis_index("cfg")
    core = lax.rem(me, CORES)
    chip = lax.div(me, CORES)
    partner = chip * CORES + (CORES - 1 - core)
    scale = LOG2E * HEAD_DIM ** (-0.5)
    last = group - 1
    half = chips // 2
    bf16 = jnp.bfloat16
    f32 = jnp.float32

    def cols(owner, head):
        return pl.ds(pl.multiple_of((owner * group + head) * HEAD_DIM, HEAD_DIM), HEAD_DIM)

    def out_cols(side, branch):
        return pl.ds(pl.multiple_of((side * 2 + branch) * wide, HEAD_DIM), wide)

    def slot(index):
        return pl.ds(pl.multiple_of(index * rows, 16), rows)

    def chip_at(step):
        return lax.rem(chip + step, chips)

    mid = chips // 2
    late = mid - lax.div(chip, mid)
    gap = lax.rem(chip + chips - late, chips)
    at_end = lax.rem(chip, chips - 1) == 0
    inside = lax.rem(chip, chips - 1) != 0

    def source(place):
        other = lax.rem(late + place + lax.div(place + chips - gap, chips), chips)
        return jnp.where(place == 0, chip, other)

    def step_from(other):
        return lax.rem(chip + chips - other, chips)

    def step_to(other):
        return lax.rem(other + chips - chip, chips)

    def chip_back(step):
        return lax.rem(chip + chips - step, chips)

    def across(src, dst, sends, recvs, device):
        return pltpu.make_async_remote_copy(
            src_ref=src, dst_ref=dst, send_sem=sends, recv_sem=recvs,
            device_id=device, device_id_type=MESH,
        )

    def drain(ref, sem):
        pltpu.make_async_copy(ref, ref, sem).wait()

    def blocks_of(number):
        return kb.at[0, pl.ds(0, number * rows)]

    x_side = {"tp": 1 - t}
    y_side = {"cfg": 1 - c}

    def kv_copies(head, step):
        target = chip_at(step)
        return [
            across(
                src.at[:, cols(target, head)], dst.at[head, slot(me)],
                send.at[head], krecv.at[head, step - 1], {"seq": target * CORES + core},
            )
            for src, dst in ((k, kb), (v, vb))
        ]

    def q_copy(head, step):
        target = chip_at(step)
        return across(
            q.at[:, cols(target, head)], qb.at[head, chip],
            send.at[head], qrecv.at[head, step - 1], {"seq": target * CORES + core},
        )

    def own_copies(head):
        return [
            pltpu.make_async_copy(k.at[:, cols(chip, head)], kb.at[head, slot(me)], local.at[head]),
            pltpu.make_async_copy(v.at[:, cols(chip, head)], vb.at[head, slot(me)], local.at[head]),
            pltpu.make_async_copy(q.at[:, cols(chip, head)], qb.at[head, chip], local.at[head]),
            pltpu.make_async_copy(tk.at[:, cols(chip, head)], tkb.at[head], local.at[head]),
            pltpu.make_async_copy(tv.at[:, cols(chip, head)], tvb.at[head], local.at[head]),
        ]

    def own_forward(head):
        return [
            across(
                src.at[:, cols(chip, head)], dst.at[head, slot(me)],
                send.at[head], frecv.at[head], {"seq": partner},
            )
            for src, dst in ((k, kb), (v, vb))
        ]

    def forwards(head, step):
        span = slot(chip_back(step) * CORES + core)
        return [
            across(
                buf.at[head, span], buf.at[head, span], send.at[head], frecv.at[head],
                {"seq": partner},
            )
            for buf in (kb, vb)
        ]

    def count_copy(step):
        return across(
            mc, cb.at[me], count.at[0], count.at[1],
            {"seq": lax.rem(me + step, n)},
        )

    def out_copy(head, step):
        target = chip_at(step)
        return across(
            ob.at[head, target], ab.at[c, t, head, chip],
            send.at[head], orecv.at[head, step], {"seq": target * CORES + core},
        )

    def own_out(head):
        return pltpu.make_async_copy(
            ob.at[head, chip], ab.at[c, t, head, chip], orecv.at[head, 0]
        )

    def arrived(head, place, odd):
        if place % 2 == odd:
            return passed.at[head, place // (chips - 1)]
        return direct.at[head]

    def x_copy(head, place):
        piece = ab.at[c, t, head, source(place)]
        return across(piece, piece, send.at[head], arrived(head, place, 1), x_side)

    def y_copy(head, place):
        piece = ab.at[c, t, head, source(place)]
        return across(piece, piece, send.at[head], arrived(head, place, 0), y_side)

    def relay(head, place):
        if place % 2 == 0:
            piece = ab.at[1 - c, t, head, source(place)]
            side = x_side
        else:
            piece = ab.at[c, 1 - t, head, source(place)]
            side = y_side
        return across(piece, piece, send.at[head], relayed.at[head], side)

    def w_own(head):
        return pltpu.make_async_copy(
            w.at[:, head, :, out_cols(t, c)], wb.at[head, t], wsem.at[0]
        )

    def w_copy(head):
        part = pl.ds(core * half, half)
        return across(
            w.at[part, head, :, out_cols(1 - t, c)], wb.at[head, t, part],
            wsem.at[3], wsem.at[1], x_side,
        )

    def w_forward(head):
        place = wb.at[head, 1 - t, pl.ds(core * half, half)]
        return across(place, place, wsem.at[3], wsem.at[2], {"seq": partner})

    parts = wide // part

    def stat_copy(turn, step):
        span = (pl.ds(0, parts - 1), pl.ds(parts - 1, 1))[turn]
        return across(
            st.at[span], sg.at[me, span], stat.at[0], stat.at[1],
            {"seq": lax.rem(me + step, n)},
        )

    mc[...] = jnp.full(mc.shape, counts[0], jnp.int32)
    barrier = pltpu.get_barrier_semaphore()
    for step in range(1, n):
        pl.semaphore_signal(
            barrier, inc=1, device_id={"seq": lax.rem(me + step, n)}, device_id_type=MESH
        )
    pl.semaphore_signal(barrier, inc=1, device_id=x_side, device_id_type=MESH)
    pl.semaphore_signal(barrier, inc=1, device_id=y_side, device_id_type=MESH)

    def start_own(head, _):
        for copy in own_copies(head):
            copy.start()
        w_own(head).start()
        return 0

    lax.fori_loop(0, group, start_own, 0)
    pl.semaphore_wait(barrier, n + 1)

    def start_kv(head):
        for step in range(1, chips):
            for copy in kv_copies(head, step):
                copy.start()

    def start_q(head):
        for step in range(1, chips):
            q_copy(head, step).start()

    for step in range(1, n):
        count_copy(step).start()
    start_kv(0)
    start_q(0)

    @pl.when(inside)
    def _():
        start_kv(1)


    def start_near(head, _):
        w_copy(head).start()
        for copy in own_forward(head):
            copy.start()
        return 0

    lax.fori_loop(0, group, start_near, 0)

    cb[me] = mc[...]
    st[...] = jnp.zeros_like(st)
    acc[...] = jnp.zeros_like(acc)
    drain(cb.at[pl.ds(0, n - 1)], count.at[1])
    lane = lax.broadcasted_iota(jnp.int32, (rows, HEAD_DIM), 1)
    place_in = lax.broadcasted_iota(jnp.int32, (rows, HEAD_DIM), 0)

    def fill_bias(source, _):
        limit = cb[source][0:1, :]
        bias[slot(source), :] = jnp.where(
            (lane == 0) & (place_in >= limit), NEGATIVE, 0.0
        ).astype(bf16)
        return 0

    lax.fori_loop(0, n, fill_bias, 0)
    tlane = lax.broadcasted_iota(jnp.int32, (text, HEAD_DIM), 1)
    tplace = lax.broadcasted_iota(jnp.int32, (text, HEAD_DIM), 0)
    tbias[...] = jnp.where(
        (tlane == 0) & (tplace >= lengths[0]), NEGATIVE, 0.0
    ).astype(bf16)

    total = n * rows
    size = chunk_rows(total, 768)

    def ones(length):
        return jnp.where(
            lax.broadcasted_iota(jnp.int32, (length, HEAD_DIM), 1) == 0, 1.0, 0.0
        ).astype(bf16)

    def one_block(head, target):
        query = jnp.concatenate([qb[head, target], ones(rows)], axis=1)

        def piece(state, keys, masks, vals):
            keys = jnp.concatenate([keys, masks], axis=1)
            vals = jnp.concatenate([vals, ones(vals.shape[0])], axis=1)
            scores = lax.dot_general(
                query, keys, (((1,), (1,)), ((), ())), preferred_element_type=f32
            )
            high = jnp.max(scores, axis=1, keepdims=True) * scale
            if state is not None:
                high = jnp.maximum(high, state[0])
            weights = jnp.exp2(scores * scale - high).astype(bf16)
            mixed = jnp.dot(weights, vals, preferred_element_type=f32)
            if state is not None:
                mixed = mixed + state[1] * jnp.exp2(state[0] - high)
            return (high, mixed)

        state = piece(None, tkb[head], tbias[...], tvb[head])
        for start in range(0, total, size):
            span = pl.ds(start, size)
            state = piece(state, kb[head, span], bias[span, :], vb[head, span])
        mixed = state[1]
        ob[head, target] = (
            mixed[:, :HEAD_DIM] / mixed[:, HEAD_DIM:HEAD_DIM + 1]
        ).astype(bf16)

    def take_keys(head):
        drain(kb.at[0, pl.ds(0, 3 * rows + 2 * text)], local.at[head])
        for step in range(1, chips):
            drain(blocks_of(2), krecv.at[head, step - 1])
            for copy in forwards(head, step):
                copy.start()
        drain(blocks_of(n), frecv.at[head])

    def share_piece(head, place):
        if place == 0:
            own_out(head).wait()
        else:
            out_copy(head, step_from(source(place))).wait_recv()
        x_copy(head, place).start()
        y_copy(head, place).start()

    def share(head, places):
        for place in places:
            share_piece(head, place)

    def pass_early(head):
        drain(blocks_of(chips - 1), passed.at[head, 0])
        for place in range(chips - 1):
            relay(head, place).start()

    def pass_late(head):
        drain(blocks_of(1), passed.at[head, 1])
        relay(head, chips - 1).start()

    def blocks(head, after):
        def block(place, _):
            other = source(place)
            far = place > 0

            @pl.when(far)
            def _():
                q_copy(head, step_from(other)).wait_recv()

            if after is None:
                @pl.when((place == chips - 1) & at_end)
                def _():
                    start_kv(head + 1)

            one_block(head, other)

            @pl.when(far)
            def _():
                out_copy(head, step_to(other)).start()

            @pl.when(place == 0)
            def _():
                own_out(head).start()
                share_piece(head, 0)

            if after is not None:
                after(place)
            return 0

        lax.fori_loop(0, chips, block, 0)

    def collect_direct(head):
        drain(blocks_of(chips), direct.at[head])

    def collect_relayed(head):
        drain(blocks_of(chips), relayed.at[head])

    def collect(head):
        collect_direct(head)
        collect_relayed(head)

    depth = 2 * chips * HEAD_DIM

    def product(head, branch, span):
        rows_in = jnp.concatenate(
            [ab[branch, side, head, source] for side in range(2) for source in range(chips)],
            axis=1,
        )
        weight = wb[head, :, :, :, span].reshape(depth, part)
        return jnp.dot(rows_in, weight, preferred_element_type=f32)

    def side_product(head, branch, side, span):
        rows_in = jnp.concatenate(
            [ab[branch, side, head, source] for source in range(chips)], axis=1
        )
        weight = wb[head, side, :, :, span].reshape(chips * HEAD_DIM, part)
        return jnp.dot(rows_in, weight, preferred_element_type=f32)

    def span_of(index):
        return pl.ds(pl.multiple_of(index * part, HEAD_DIM), part)

    def project(head):
        def one(index, _):
            span = span_of(index)
            for branch in range(2):
                acc[branch, :, span] += product(head, branch, span)
            return 0

        lax.fori_loop(0, parts, one, 0)

    def project_side(head, branch, side):
        def one(index, _):
            span = span_of(index)
            acc[branch, :, span] += side_product(head, branch, side, span)
            return 0

        lax.fori_loop(0, parts, one, 0)

    near = pl.ds(0, half)

    def pass_weight(index, _):
        w_forward(index).start()
        return 0

    def one_head(head, _):
        take_keys(head)
        blocks(head, None)
        start_q(head + 1)

        @pl.when(inside & (head + 2 <= last))
        def _():
            start_kv(head + 2)

        @pl.when(head == 1)
        def _():
            drain(wb.at[:, 0, near], wsem.at[1])
            lax.fori_loop(0, group, pass_weight, 0)

        @pl.when(head >= 1)
        def _():
            pass_early(head - 1)
            pass_late(head - 1)

        @pl.when(head + 1 < last)
        def _():
            share(head, range(1, chips))

        @pl.when(head == 1)
        def _():
            drain(wb.at[:, 0], wsem.at[0])
            drain(wb.at[:, 0, near], wsem.at[2])

        @pl.when(head >= 1)
        def _():
            collect(head - 1)
            project(head - 1)

        return 0

    lax.fori_loop(0, last, one_head, 0)
    share(last - 1, range(1, chips - 1))
    take_keys(last)

    def after_block(place):
        @pl.when(place == 0)
        def _():
            share_piece(last - 1, chips - 1)
            pass_early(last - 1)

        @pl.when(place == chips - 2)
        def _():
            pass_late(last - 1)

    blocks(last, after_block)
    collect(last - 1)
    project(last - 1)
    share(last, range(1, chips))
    project_side(last, c, t)
    pass_early(last)
    pass_late(last)
    collect_direct(last)
    project_side(last, c, 1 - t)
    project_side(last, 1 - c, t)
    collect_relayed(last)

    limit = cb[me][0:1, 0:1]
    valid = lax.broadcasted_iota(jnp.int32, (rows, part), 0) < limit
    first = jnp.full((rows, part), c, jnp.int32) == 0
    pairs = part // HEAD_DIM

    def guide(index, _):
        span = span_of(index)
        mine = acc[c, :, span].astype(bf16).astype(f32)
        other = acc[1 - c, :, span] + side_product(last, 1 - c, 1 - t, span)
        other = other.astype(bf16).astype(f32)
        conditional = jnp.where(first, mine, other)
        unconditional = jnp.where(first, other, mine)
        guided = unconditional + GUIDANCE * (conditional - unconditional)
        acc[0, :, span] = guided
        guided = jnp.where(valid, guided, 0.0)
        conditional = jnp.where(valid, conditional, 0.0)
        for row, field in enumerate(
            (guided, guided * guided, conditional, conditional * conditional)
        ):
            total_row = jnp.sum(field, axis=0, keepdims=True)
            for pair in range(pairs):
                st[index, 4 * pair + row:4 * pair + row + 1, :] = total_row[
                    :, pair * HEAD_DIM:(pair + 1) * HEAD_DIM
                ]

        @pl.when(index == parts - 2)
        def _():
            for step in range(1, n):
                stat_copy(0, step).start()

        return 0

    lax.fori_loop(0, parts, guide, 0)
    for step in range(1, n):
        stat_copy(1, step).start()

    def settle(head, _):
        drain(kb.at[pl.ds(0, chips)], send.at[head])
        return 0

    lax.fori_loop(0, group, settle, 0)
    drain(wb.at[:, 0], wsem.at[3])
    drain(cb.at[pl.ds(0, n - 1)], count.at[0])
    valid_total = cb[0][0:1, :]
    for source in range(1, n):
        valid_total = valid_total + cb[source][0:1, :]
    valid_total = valid_total.astype(f32)

    def store(index):
        return pltpu.make_async_copy(vel.at[index], out.at[:, span_of(index)], vsem.at[0])

    drain(sg.at[pl.ds(0, n - 1)], stat.at[1])

    def finish(index, _):
        sums = st[index]
        for step in range(1, n):
            sums = sums + sg[lax.rem(me + step, n), index]
        for pair in range(pairs):
            here = sums[4 * pair:4 * pair + 4] / valid_total
            guided_mean = here[0:1, :]
            guided_var = here[1:2, :] - guided_mean * guided_mean
            cond_mean = here[2:3, :]
            cond_var = here[3:4, :] - cond_mean * cond_mean
            std_ratio = jnp.sqrt((cond_var + 1.0) / (guided_var + 1.0))
            factor = RESCALE * std_ratio + (1.0 - RESCALE)
            span = pl.ds(pl.multiple_of(index * part + pair * HEAD_DIM, HEAD_DIM), HEAD_DIM)
            vel[index, :, pair * HEAD_DIM:(pair + 1) * HEAD_DIM] = (
                guided_mean + (acc[0, :, span] - guided_mean) * factor
            ).astype(bf16)
        store(index).start()
        return 0

    lax.fori_loop(0, parts, finish, 0)

    drain(sg.at[pl.ds(0, n - 1)], stat.at[0])
    drain(vel, vsem.at[0])


def fused_step(
    queries, keys, values, text_keys, text_values, prompt_lengths, frame_counts, out_weight, n
):
    rows, width = queries.shape
    text = text_keys.shape[0]
    chips = n // CORES
    heads = width // HEAD_DIM
    group = heads // chips
    wide = out_weight.shape[1] // 4
    part = 256 if wide % 256 == 0 else HEAD_DIM
    parts = wide // part
    weight = out_weight.reshape(chips, group, HEAD_DIM, out_weight.shape[1])
    bf16 = jnp.bfloat16
    f32 = jnp.float32
    total = n * rows
    hbm = pl.BlockSpec(memory_space=pl.ANY)
    smem = pl.BlockSpec(memory_space=pltpu.SMEM)
    dma = pltpu.SemaphoreType.DMA
    return pl.pallas_call(
        functools.partial(step_kernel, n, chips, group, rows, text, wide, part),
        out_shape=jax.ShapeDtypeStruct((rows, wide), bf16),
        in_specs=[hbm] * 6 + [smem] * 2,
        out_specs=hbm,
        scratch_shapes=[
            pltpu.VMEM((group, chips, rows, HEAD_DIM), bf16),
            pltpu.VMEM((group, total, HEAD_DIM), bf16),
            pltpu.VMEM((group, total, HEAD_DIM), bf16),
            pltpu.VMEM((group, text, HEAD_DIM), bf16),
            pltpu.VMEM((group, text, HEAD_DIM), bf16),
            pltpu.VMEM((8, HEAD_DIM), jnp.int32),
            pltpu.VMEM((n, 8, HEAD_DIM), jnp.int32),
            pltpu.VMEM((total, HEAD_DIM), bf16),
            pltpu.VMEM((text, HEAD_DIM), bf16),
            pltpu.VMEM((group, chips, rows, HEAD_DIM), bf16),
            pltpu.VMEM((2, 2, group, chips, rows, HEAD_DIM), bf16),
            pltpu.VMEM((group, 2, chips, HEAD_DIM, wide), bf16),
            pltpu.VMEM((2, rows, wide), f32),
            pltpu.VMEM((parts, 8, HEAD_DIM), f32),
            pltpu.VMEM((n, parts, 8, HEAD_DIM), f32),
            pltpu.VMEM((parts, rows, part), bf16),
            dma((group,)),
            dma((group, chips - 1)),
            dma((group, chips - 1)),
            dma((group,)),
            dma((2,)),
            dma((group,)),
            dma((group, chips)),
            dma((group, 2)),
            dma((group,)),
            dma((group,)),
            dma((4,)),
            dma((2,)),
            dma((1,)),
        ],
        compiler_params=pltpu.CompilerParams(
            collective_id=0, has_side_effects=True, vmem_limit_bytes=62 * 1024 * 1024
        ),
    )(queries, keys, values, text_keys, text_values, weight, frame_counts, prompt_lengths)


def frame_valid(positions, counts_table, slots):
    frame_index = positions // slots
    slot_index = positions % slots
    frame_ids = jnp.arange(counts_table.shape[0], dtype=jnp.int32)
    frame_limit = jnp.sum(
        jnp.where(frame_index[:, None] == frame_ids[None, :], counts_table[None, :], 0), axis=1
    )
    return slot_index < frame_limit


def attend_block(carry, key_rows, value_rows, query_heads, key_mask):
    row_max, weight_sum, mixed_sum = carry
    head_count = query_heads.shape[1]
    key_heads = key_rows.reshape(key_rows.shape[0], head_count, HEAD_DIM)
    value_heads = value_rows.reshape(value_rows.shape[0], head_count, HEAD_DIM)
    scores = jnp.einsum(
        "qhd,khd->hqk", query_heads, key_heads, preferred_element_type=jnp.float32
    ) * HEAD_DIM ** (-0.5)
    scores = jnp.where(key_mask[None, None, :], scores, NEGATIVE)
    new_max = jnp.maximum(row_max, jnp.max(scores, axis=2))
    shrink = jnp.exp(row_max - new_max)
    weights = jnp.exp(scores - new_max[:, :, None])
    weight_sum = weight_sum * shrink + jnp.sum(weights, axis=2)
    mixed_sum = mixed_sum * shrink[:, :, None] + jnp.einsum(
        "hqk,khd->hqd",
        weights.astype(jnp.bfloat16),
        value_heads,
        preferred_element_type=jnp.float32,
    )
    return (new_max, weight_sum, mixed_sum)


def gathered_attention(
    queries, keys, values, text_keys, text_values, prompt_lengths, frame_counts, n
):
    row_count, head_cols = queries.shape
    head_count = head_cols // HEAD_DIM
    all_counts = lax.all_gather(frame_counts, "seq", axis=0, tiled=True)
    query_heads = queries.reshape(row_count, head_count, HEAD_DIM)
    text_mask = jnp.arange(text_keys.shape[0], dtype=jnp.int32) < prompt_lengths[0]
    empty_state = (
        jnp.full((head_count, row_count), NEGATIVE, jnp.float32),
        jnp.zeros((head_count, row_count), jnp.float32),
        jnp.zeros((head_count, row_count, HEAD_DIM), jnp.float32),
    )
    text_state = attend_block(empty_state, text_keys, text_values, query_heads, text_mask)
    key_rows = lax.all_gather(keys, "seq", axis=0, tiled=True)
    value_rows = lax.all_gather(values, "seq", axis=0, tiled=True)
    positions = jnp.arange(key_rows.shape[0], dtype=jnp.int32)
    _, weight_sum, mixed_sum = attend_block(
        text_state, key_rows, value_rows, query_heads,
        frame_valid(positions, all_counts, row_count // frame_counts.shape[0]),
    )
    return (
        jnp.transpose(mixed_sum / weight_sum[:, :, None], (1, 0, 2))
        .reshape(row_count, head_cols)
        .astype(jnp.bfloat16)
    )


def fits_fused(n, cfgs, tps, queries, text_keys, frame_counts, out_weight):
    heads = queries.shape[2] // HEAD_DIM
    chips = n // CORES
    if cfgs != 2 or tps != 2 or n % CORES or frame_counts.shape[0] != 1:
        return False
    if chips != 4 or heads % chips or heads // chips < 4:
        return False
    if 3 * queries.shape[1] + 2 * text_keys.shape[1] > n * queries.shape[1]:
        return False
    return out_weight.shape[1] % (8 * HEAD_DIM) == 0 and queries.shape[1] % 16 == 0


def body(n, cfgs, tps, queries, keys, values, text_keys, text_values, prompt_lengths, frame_counts, out_weight):
    rows = queries.shape[1]
    if fits_fused(n, cfgs, tps, queries, text_keys, frame_counts, out_weight):
        return fused_step(
            queries[0], keys[0], values[0], text_keys[0], text_values[0],
            prompt_lengths, frame_counts, out_weight, n,
        )
    attended = gathered_attention(
        queries[0], keys[0], values[0], text_keys[0], text_values[0],
        prompt_lengths, frame_counts, n,
    )
    branch = lax.psum_scatter(
        lax.dot_general(
            out_weight, attended, (((0,), (1,)), ((), ())), preferred_element_type=jnp.float32
        ).astype(jnp.bfloat16),
        "tp",
        scatter_dimension=0,
        tiled=True,
    )
    half = branch.shape[0] // cfgs
    mine = lax.axis_index("cfg")
    kept = lax.dynamic_slice_in_dim(branch, mine * half, half, 0)
    given = lax.dynamic_slice_in_dim(branch, (1 - mine) * half, half, 0)
    other = lax.ppermute(given, "cfg", [(0, 1), (1, 0)])
    first = mine == 0
    conditional = jnp.where(first, kept, other).astype(jnp.float32)
    unconditional = jnp.where(first, other, kept).astype(jnp.float32)
    guided = unconditional + GUIDANCE * (conditional - unconditional)
    valid = (jnp.arange(rows, dtype=jnp.int32) < frame_counts[0])[None, :]

    def local_sum(field):
        return jnp.sum(jnp.where(valid, field, 0.0), axis=1)

    sums = lax.psum(
        jnp.stack([
            local_sum(guided),
            local_sum(guided * guided),
            local_sum(conditional),
            local_sum(conditional * conditional),
            jnp.full((half,), frame_counts[0].astype(jnp.float32)),
        ]),
        "seq",
    )
    means = sums[:4] / sums[4:5]
    guided_mean = means[0]
    guided_var = means[1] - guided_mean * guided_mean
    cond_var = means[3] - means[2] * means[2]
    std_ratio = jnp.sqrt((cond_var + 1.0) / (guided_var + 1.0))
    factor = RESCALE * std_ratio + (1.0 - RESCALE)
    velocity = guided_mean[:, None] + (guided - guided_mean[:, None]) * factor[:, None]
    return velocity.astype(jnp.bfloat16).T


def solution(mesh):
    placed = (
        P("cfg", "seq", "tp"),
        P("cfg", "seq", "tp"),
        P("cfg", "seq", "tp"),
        P("cfg", None, "tp"),
        P("cfg", None, "tp"),
        P("cfg"),
        P("seq"),
        P("tp", None),
    )
    return jax.shard_map(
        functools.partial(body, mesh.shape["seq"], mesh.shape["cfg"], mesh.shape["tp"]),
        mesh=mesh, in_specs=placed, out_specs=P("seq", ("tp", "cfg")), check_vma=False,
    )
```

```python
import functools

import jax
import jax.numpy as jnp
from jax import lax
from jax.experimental import pallas as pl
from jax.experimental.pallas import tpu as pltpu
from jax.sharding import PartitionSpec as P

HEAD_DIM = 128
GUIDANCE = 5.0
RESCALE = 0.7
NEGATIVE = -1e30
LOG2E = 1.4426950408889634
CORES = 2
MESH = pl.DeviceIdType.MESH


def chunk_rows(total, limit):
    for unit in (256, 128, 16):
        for size in range(limit // unit * unit, 0, -unit):
            if total % size == 0:
                return size
    return total


def step_kernel(
    n, chips, group, rows, text, wide, part,
    q, k, v, tk, tv, w, counts, lengths,
    out,
    qb, kb, vb, tkb, tvb, mc, cb, bias, tbias, ob, ab, wb, acc, st, sg, vel,
    send, krecv, qrecv, frecv, count, local, orecv, passed, direct, relayed, wsem, stat, vsem,
):
    me = lax.axis_index("seq")
    t = lax.axis_index("tp")
    c = lax.axis_index("cfg")
    core = lax.rem(me, CORES)
    chip = lax.div(me, CORES)
    partner = chip * CORES + (CORES - 1 - core)
    scale = LOG2E * HEAD_DIM ** (-0.5)
    last = group - 1
    half = chips // 2
    bf16 = jnp.bfloat16
    f32 = jnp.float32

    def cols(owner, head):
        return pl.ds(pl.multiple_of((owner * group + head) * HEAD_DIM, HEAD_DIM), HEAD_DIM)

    def out_cols(side, branch):
        return pl.ds(pl.multiple_of((side * 2 + branch) * wide, HEAD_DIM), wide)

    def slot(index):
        return pl.ds(pl.multiple_of(index * rows, 16), rows)

    def chip_at(step):
        return lax.rem(chip + step, chips)

    mid = chips // 2
    upper = lax.div(chip, mid)
    lower = 1 - upper
    gap = lax.rem(upper * chip + lower * (chips - 1 - chip) + chips + 1 - mid, chips)
    at_end = lax.rem(chip, chips - 1) == 0
    inside = lax.rem(chip, chips - 1) != 0

    def source(place):
        other = lax.rem(mid - 1 + place + lax.div(place + chips - gap, chips), chips)
        other = upper * other + lower * (chips - 1 - other)
        return jnp.where(place == 0, chip, other)

    def turned(step):
        return upper * step + lower * (chips - step)

    def step_from(other):
        return lax.rem(chip + chips - other, chips)

    def step_to(other):
        return lax.rem(other + chips - chip, chips)

    def chip_back(step):
        return lax.rem(chip + chips - step, chips)

    def across(src, dst, sends, recvs, device):
        return pltpu.make_async_remote_copy(
            src_ref=src, dst_ref=dst, send_sem=sends, recv_sem=recvs,
            device_id=device, device_id_type=MESH,
        )

    def drain(ref, sem):
        pltpu.make_async_copy(ref, ref, sem).wait()

    def blocks_of(number):
        return kb.at[0, pl.ds(0, number * rows)]

    x_side = {"tp": 1 - t}
    y_side = {"cfg": 1 - c}

    def kv_copies(head, step):
        target = chip_at(step)
        return [
            across(
                src.at[:, cols(target, head)], dst.at[head, slot(me)],
                send.at[head], krecv.at[head, step - 1], {"seq": target * CORES + core},
            )
            for src, dst in ((k, kb), (v, vb))
        ]

    def q_copy(head, step):
        target = chip_at(step)
        return across(
            q.at[:, cols(target, head)], qb.at[head, chip],
            send.at[head], qrecv.at[head, step - 1], {"seq": target * CORES + core},
        )

    def own_copies(head):
        return [
            pltpu.make_async_copy(k.at[:, cols(chip, head)], kb.at[head, slot(me)], local.at[head]),
            pltpu.make_async_copy(v.at[:, cols(chip, head)], vb.at[head, slot(me)], local.at[head]),
            pltpu.make_async_copy(q.at[:, cols(chip, head)], qb.at[head, chip], local.at[head]),
            pltpu.make_async_copy(tk.at[:, cols(chip, head)], tkb.at[head], local.at[head]),
            pltpu.make_async_copy(tv.at[:, cols(chip, head)], tvb.at[head], local.at[head]),
        ]

    def own_forward(head):
        return [
            across(
                src.at[:, cols(chip, head)], dst.at[head, slot(me)],
                send.at[head], frecv.at[head], {"seq": partner},
            )
            for src, dst in ((k, kb), (v, vb))
        ]

    def forwards(head, step):
        span = slot(chip_back(step) * CORES + core)
        return [
            across(
                buf.at[head, span], buf.at[head, span], send.at[head], frecv.at[head],
                {"seq": partner},
            )
            for buf in (kb, vb)
        ]

    def count_copy(step):
        return across(
            mc, cb.at[me], count.at[0], count.at[1],
            {"seq": lax.rem(me + step, n)},
        )

    def out_copy(head, step):
        target = chip_at(step)
        return across(
            ob.at[head, target], ab.at[c, t, head, chip],
            send.at[head], orecv.at[head, step], {"seq": target * CORES + core},
        )

    def own_out(head):
        return pltpu.make_async_copy(
            ob.at[head, chip], ab.at[c, t, head, chip], orecv.at[head, 0]
        )

    def arrived(head, place, turn):
        if place // half == turn:
            return passed.at[head, place]
        return direct.at[head]

    def x_copy(head, place):
        piece = ab.at[c, t, head, source(place)]
        return across(piece, piece, send.at[head], arrived(head, place, 1), x_side)

    def y_copy(head, place):
        piece = ab.at[c, t, head, source(place)]
        return across(piece, piece, send.at[head], arrived(head, place, 0), y_side)

    def relay(head, place):
        if place < half:
            piece = ab.at[1 - c, t, head, source(place)]
            side = x_side
        else:
            piece = ab.at[c, 1 - t, head, source(place)]
            side = y_side
        return across(piece, piece, send.at[head], relayed.at[head], side)

    def w_own(head):
        return pltpu.make_async_copy(
            w.at[:, head, :, out_cols(t, c)], wb.at[head, t], wsem.at[0]
        )

    def w_copy(head):
        part = pl.ds(core * half, half)
        return across(
            w.at[part, head, :, out_cols(1 - t, c)], wb.at[head, t, part],
            wsem.at[3], wsem.at[1], x_side,
        )

    def w_forward(head):
        place = wb.at[head, 1 - t, pl.ds(core * half, half)]
        return across(place, place, wsem.at[3], wsem.at[2], {"seq": partner})

    parts = wide // part

    def stat_copy(turn, step):
        span = (pl.ds(0, parts - 1), pl.ds(parts - 1, 1))[turn]
        return across(
            st.at[span], sg.at[me, span], stat.at[0], stat.at[1],
            {"seq": lax.rem(me + step, n)},
        )

    mc[...] = jnp.full(mc.shape, counts[0], jnp.int32)
    barrier = pltpu.get_barrier_semaphore()
    for step in range(1, n):
        pl.semaphore_signal(
            barrier, inc=1, device_id={"seq": lax.rem(me + step, n)}, device_id_type=MESH
        )
    pl.semaphore_signal(barrier, inc=1, device_id=x_side, device_id_type=MESH)
    pl.semaphore_signal(barrier, inc=1, device_id=y_side, device_id_type=MESH)

    def start_own(head, _):
        for copy in own_copies(head):
            copy.start()
        w_own(head).start()
        return 0

    lax.fori_loop(0, group, start_own, 0)
    pl.semaphore_wait(barrier, n + 1)

    def start_kv(head):
        for step in range(1, chips):
            for copy in kv_copies(head, turned(step)):
                copy.start()

    def start_q(head):
        for step in range(1, chips):
            q_copy(head, turned(step)).start()

    for step in range(1, n):
        count_copy(step).start()
    start_kv(0)
    start_q(0)

    @pl.when(inside)
    def _():
        start_kv(1)


    def start_near(head, _):
        w_copy(head).start()
        for copy in own_forward(head):
            copy.start()
        return 0

    lax.fori_loop(0, group, start_near, 0)

    cb[me] = mc[...]
    st[...] = jnp.zeros_like(st)
    acc[...] = jnp.zeros_like(acc)
    drain(cb.at[pl.ds(0, n - 1)], count.at[1])
    lane = lax.broadcasted_iota(jnp.int32, (rows, HEAD_DIM), 1)
    place_in = lax.broadcasted_iota(jnp.int32, (rows, HEAD_DIM), 0)

    def fill_bias(origin, _):
        limit = cb[origin][0:1, :]
        bias[slot(origin), :] = jnp.where(
            (lane == 0) & (place_in >= limit), NEGATIVE, 0.0
        ).astype(bf16)
        return 0

    lax.fori_loop(0, n, fill_bias, 0)
    tlane = lax.broadcasted_iota(jnp.int32, (text, HEAD_DIM), 1)
    tplace = lax.broadcasted_iota(jnp.int32, (text, HEAD_DIM), 0)
    tbias[...] = jnp.where(
        (tlane == 0) & (tplace >= lengths[0]), NEGATIVE, 0.0
    ).astype(bf16)

    total = n * rows
    size = chunk_rows(total, 768)

    def ones(length):
        return jnp.where(
            lax.broadcasted_iota(jnp.int32, (length, HEAD_DIM), 1) == 0, 1.0, 0.0
        ).astype(bf16)

    def one_block(head, target):
        query = jnp.concatenate([qb[head, target], ones(rows)], axis=1)

        def piece(state, keys, masks, vals):
            keys = jnp.concatenate([keys, masks], axis=1)
            vals = jnp.concatenate([vals, ones(vals.shape[0])], axis=1)
            scores = lax.dot_general(
                query, keys, (((1,), (1,)), ((), ())), preferred_element_type=f32
            )
            high = jnp.max(scores, axis=1, keepdims=True) * scale
            if state is not None:
                high = jnp.maximum(high, state[0])
            weights = jnp.exp2(scores * scale - high).astype(bf16)
            mixed = jnp.dot(weights, vals, preferred_element_type=f32)
            if state is not None:
                mixed = mixed + state[1] * jnp.exp2(state[0] - high)
            return (high, mixed)

        state = piece(None, tkb[head], tbias[...], tvb[head])
        for start in range(0, total, size):
            span = pl.ds(start, size)
            state = piece(state, kb[head, span], bias[span, :], vb[head, span])
        mixed = state[1]
        ob[head, target] = (
            mixed[:, :HEAD_DIM] / mixed[:, HEAD_DIM:HEAD_DIM + 1]
        ).astype(bf16)

    def take_keys(head):
        drain(kb.at[0, pl.ds(0, 3 * rows + 2 * text)], local.at[head])
        for step in range(1, chips):
            drain(blocks_of(2), krecv.at[head, turned(step) - 1])
            for copy in forwards(head, turned(step)):
                copy.start()
        drain(blocks_of(n), frecv.at[head])

    def share_piece(head, place):
        if place == 0:
            own_out(head).wait()
        else:
            out_copy(head, step_from(source(place))).wait_recv()
        x_copy(head, place).start()
        y_copy(head, place).start()

    def share(head, places):
        for place in places:
            share_piece(head, place)

    def pass_on(head, places):
        for place in places:
            drain(blocks_of(1), passed.at[head, place])
            relay(head, place).start()

    def blocks(head, after):
        def block(place, _):
            other = source(place)
            far = place > 0

            @pl.when(far)
            def _():
                q_copy(head, step_from(other)).wait_recv()

            if after is None:
                @pl.when((place == chips - 1) & at_end)
                def _():
                    start_kv(head + 1)

            one_block(head, other)

            @pl.when(far)
            def _():
                out_copy(head, step_to(other)).start()

            @pl.when(place == 0)
            def _():
                own_out(head).start()
                share_piece(head, 0)

            if after is not None:
                after(place)
            return 0

        lax.fori_loop(0, chips, block, 0)

    def collect_direct(head):
        drain(blocks_of(chips), direct.at[head])

    def collect_relayed(head):
        drain(blocks_of(chips), relayed.at[head])

    def collect(head):
        collect_direct(head)
        collect_relayed(head)

    depth = 2 * chips * HEAD_DIM

    def product(head, branch, span):
        rows_in = jnp.concatenate(
            [ab[branch, side, head, owner] for side in range(2) for owner in range(chips)],
            axis=1,
        )
        weight = wb[head, :, :, :, span].reshape(depth, part)
        return jnp.dot(rows_in, weight, preferred_element_type=f32)

    def side_product(head, branch, side, span):
        rows_in = jnp.concatenate(
            [ab[branch, side, head, owner] for owner in range(chips)], axis=1
        )
        weight = wb[head, side, :, :, span].reshape(chips * HEAD_DIM, part)
        return jnp.dot(rows_in, weight, preferred_element_type=f32)

    def span_of(index):
        return pl.ds(pl.multiple_of(index * part, HEAD_DIM), part)

    def project(head):
        def one(index, _):
            span = span_of(index)
            for branch in range(2):
                acc[branch, :, span] += product(head, branch, span)
            return 0

        lax.fori_loop(0, parts, one, 0)

    def project_branch(head, branch):
        def one(index, _):
            span = span_of(index)
            acc[branch, :, span] += product(head, branch, span)
            return 0

        lax.fori_loop(0, parts, one, 0)

    def project_side(head, branch, side):
        def one(index, _):
            span = span_of(index)
            acc[branch, :, span] += side_product(head, branch, side, span)
            return 0

        lax.fori_loop(0, parts, one, 0)

    near = pl.ds(0, half)

    def pass_weight(index, _):
        w_forward(index).start()
        return 0

    def one_head(head, _):
        take_keys(head)
        blocks(head, None)
        start_q(head + 1)

        @pl.when(inside & (head + 2 <= last))
        def _():
            start_kv(head + 2)

        @pl.when(head == 1)
        def _():
            drain(wb.at[:, 0, near], wsem.at[1])
            lax.fori_loop(0, group, pass_weight, 0)

        @pl.when(head >= 1)
        def _():
            share(head - 1, range(1, chips))

        @pl.when(head == 2)
        def _():
            drain(wb.at[:, 0], wsem.at[0])
            drain(wb.at[:, 0, near], wsem.at[2])

        @pl.when(head >= 2)
        def _():
            collect(head - 2)
            project(head - 2)

        @pl.when(head >= 1)
        def _():
            pass_on(head - 1, range(chips))

        return 0

    lax.fori_loop(0, last, one_head, 0)
    early = range(1, chips - 1)
    collect(last - 2)
    project(last - 2)
    share(last - 1, early)

    take_keys(last)

    def after_block(place):
        @pl.when(place == 0)
        def _():
            share_piece(last - 1, chips - 1)
            pass_on(last - 1, range(chips - 1))

        @pl.when(place == chips - 2)
        def _():
            pass_on(last - 1, (chips - 1,))
            pass_on(last, (0,))

    blocks(last, after_block)
    share(last, early)
    collect(last - 1)
    project(last - 1)
    share(last, (chips - 1,))
    pass_on(last, range(1, chips))
    collect_direct(last)
    project_branch(last, c)
    project_side(last, 1 - c, t)
    collect_relayed(last)

    limit = cb[me][0:1, 0:1]
    valid = lax.broadcasted_iota(jnp.int32, (rows, part), 0) < limit
    first = jnp.full((rows, part), c, jnp.int32) == 0
    pairs = part // HEAD_DIM

    def guide(index):
        span = pl.ds(index * part, part)
        mine = acc[c, :, span].astype(bf16).astype(f32)
        other = acc[1 - c, :, span] + side_product(last, 1 - c, 1 - t, span)
        other = other.astype(bf16).astype(f32)
        conditional = jnp.where(first, mine, other)
        unconditional = jnp.where(first, other, mine)
        guided = unconditional + GUIDANCE * (conditional - unconditional)
        acc[0, :, span] = guided
        guided = jnp.where(valid, guided, 0.0)
        conditional = jnp.where(valid, conditional, 0.0)
        for row, field in enumerate(
            (guided, guided * guided, conditional, conditional * conditional)
        ):
            total_row = jnp.sum(field, axis=0, keepdims=True)
            for pair in range(pairs):
                st[index, 4 * pair + row:4 * pair + row + 1, :] = total_row[
                    :, pair * HEAD_DIM:(pair + 1) * HEAD_DIM
                ]

    for index in range(parts):
        guide(index)
        if index >= parts - 2:
            for step in range(1, n):
                stat_copy(index + 2 - parts, step).start()

    def settle(head, _):
        drain(kb.at[pl.ds(0, chips)], send.at[head])
        return 0

    lax.fori_loop(0, group, settle, 0)
    drain(wb.at[:, 0], wsem.at[3])
    drain(cb.at[pl.ds(0, n - 1)], count.at[0])
    valid_total = cb[0][0:1, :]
    for origin in range(1, n):
        valid_total = valid_total + cb[origin][0:1, :]
    valid_total = valid_total.astype(f32)

    def store(index):
        return pltpu.make_async_copy(vel.at[index], out.at[:, span_of(index)], vsem.at[0])

    drain(sg.at[pl.ds(0, n - 1)], stat.at[1])

    def finish(index, _):
        sums = st[index]
        for step in range(1, n):
            sums = sums + sg[lax.rem(me + step, n), index]
        for pair in range(pairs):
            here = sums[4 * pair:4 * pair + 4] / valid_total
            guided_mean = here[0:1, :]
            guided_var = here[1:2, :] - guided_mean * guided_mean
            cond_mean = here[2:3, :]
            cond_var = here[3:4, :] - cond_mean * cond_mean
            std_ratio = jnp.sqrt((cond_var + 1.0) / (guided_var + 1.0))
            factor = RESCALE * std_ratio + (1.0 - RESCALE)
            span = pl.ds(pl.multiple_of(index * part + pair * HEAD_DIM, HEAD_DIM), HEAD_DIM)
            vel[index, :, pair * HEAD_DIM:(pair + 1) * HEAD_DIM] = (
                guided_mean + (acc[0, :, span] - guided_mean) * factor
            ).astype(bf16)
        store(index).start()
        return 0

    lax.fori_loop(0, parts, finish, 0)

    drain(sg.at[pl.ds(0, n - 1)], stat.at[0])
    drain(vel, vsem.at[0])


def fused_step(
    queries, keys, values, text_keys, text_values, prompt_lengths, frame_counts, out_weight, n
):
    rows, width = queries.shape
    text = text_keys.shape[0]
    chips = n // CORES
    heads = width // HEAD_DIM
    group = heads // chips
    wide = out_weight.shape[1] // 4
    part = 256 if wide % 256 == 0 else HEAD_DIM
    parts = wide // part
    weight = out_weight.reshape(chips, group, HEAD_DIM, out_weight.shape[1])
    bf16 = jnp.bfloat16
    f32 = jnp.float32
    total = n * rows
    hbm = pl.BlockSpec(memory_space=pl.ANY)
    smem = pl.BlockSpec(memory_space=pltpu.SMEM)
    dma = pltpu.SemaphoreType.DMA
    return pl.pallas_call(
        functools.partial(step_kernel, n, chips, group, rows, text, wide, part),
        out_shape=jax.ShapeDtypeStruct((rows, wide), bf16),
        in_specs=[hbm] * 6 + [smem] * 2,
        out_specs=hbm,
        scratch_shapes=[
            pltpu.VMEM((group, chips, rows, HEAD_DIM), bf16),
            pltpu.VMEM((group, total, HEAD_DIM), bf16),
            pltpu.VMEM((group, total, HEAD_DIM), bf16),
            pltpu.VMEM((group, text, HEAD_DIM), bf16),
            pltpu.VMEM((group, text, HEAD_DIM), bf16),
            pltpu.VMEM((8, HEAD_DIM), jnp.int32),
            pltpu.VMEM((n, 8, HEAD_DIM), jnp.int32),
            pltpu.VMEM((total, HEAD_DIM), bf16),
            pltpu.VMEM((text, HEAD_DIM), bf16),
            pltpu.VMEM((group, chips, rows, HEAD_DIM), bf16),
            pltpu.VMEM((2, 2, group, chips, rows, HEAD_DIM), bf16),
            pltpu.VMEM((group, 2, chips, HEAD_DIM, wide), bf16),
            pltpu.VMEM((2, rows, wide), f32),
            pltpu.VMEM((parts, 8, HEAD_DIM), f32),
            pltpu.VMEM((n, parts, 8, HEAD_DIM), f32),
            pltpu.VMEM((parts, rows, part), bf16),
            dma((group,)),
            dma((group, chips - 1)),
            dma((group, chips - 1)),
            dma((group,)),
            dma((2,)),
            dma((group,)),
            dma((group, chips)),
            dma((group, chips)),
            dma((group,)),
            dma((group,)),
            dma((4,)),
            dma((2,)),
            dma((1,)),
        ],
        compiler_params=pltpu.CompilerParams(
            collective_id=0, has_side_effects=True, vmem_limit_bytes=52 * 1024 * 1024
        ),
    )(queries, keys, values, text_keys, text_values, weight, frame_counts, prompt_lengths)


def frame_valid(positions, counts_table, slots):
    frame_index = positions // slots
    slot_index = positions % slots
    frame_ids = jnp.arange(counts_table.shape[0], dtype=jnp.int32)
    frame_limit = jnp.sum(
        jnp.where(frame_index[:, None] == frame_ids[None, :], counts_table[None, :], 0), axis=1
    )
    return slot_index < frame_limit


def attend_block(carry, key_rows, value_rows, query_heads, key_mask):
    row_max, weight_sum, mixed_sum = carry
    head_count = query_heads.shape[1]
    key_heads = key_rows.reshape(key_rows.shape[0], head_count, HEAD_DIM)
    value_heads = value_rows.reshape(value_rows.shape[0], head_count, HEAD_DIM)
    scores = jnp.einsum(
        "qhd,khd->hqk", query_heads, key_heads, preferred_element_type=jnp.float32
    ) * HEAD_DIM ** (-0.5)
    scores = jnp.where(key_mask[None, None, :], scores, NEGATIVE)
    new_max = jnp.maximum(row_max, jnp.max(scores, axis=2))
    shrink = jnp.exp(row_max - new_max)
    weights = jnp.exp(scores - new_max[:, :, None])
    weight_sum = weight_sum * shrink + jnp.sum(weights, axis=2)
    mixed_sum = mixed_sum * shrink[:, :, None] + jnp.einsum(
        "hqk,khd->hqd",
        weights.astype(jnp.bfloat16),
        value_heads,
        preferred_element_type=jnp.float32,
    )
    return (new_max, weight_sum, mixed_sum)


def gathered_attention(
    queries, keys, values, text_keys, text_values, prompt_lengths, frame_counts, n
):
    row_count, head_cols = queries.shape
    head_count = head_cols // HEAD_DIM
    all_counts = lax.all_gather(frame_counts, "seq", axis=0, tiled=True)
    query_heads = queries.reshape(row_count, head_count, HEAD_DIM)
    text_mask = jnp.arange(text_keys.shape[0], dtype=jnp.int32) < prompt_lengths[0]
    empty_state = (
        jnp.full((head_count, row_count), NEGATIVE, jnp.float32),
        jnp.zeros((head_count, row_count), jnp.float32),
        jnp.zeros((head_count, row_count, HEAD_DIM), jnp.float32),
    )
    text_state = attend_block(empty_state, text_keys, text_values, query_heads, text_mask)
    key_rows = lax.all_gather(keys, "seq", axis=0, tiled=True)
    value_rows = lax.all_gather(values, "seq", axis=0, tiled=True)
    positions = jnp.arange(key_rows.shape[0], dtype=jnp.int32)
    _, weight_sum, mixed_sum = attend_block(
        text_state, key_rows, value_rows, query_heads,
        frame_valid(positions, all_counts, row_count // frame_counts.shape[0]),
    )
    return (
        jnp.transpose(mixed_sum / weight_sum[:, :, None], (1, 0, 2))
        .reshape(row_count, head_cols)
        .astype(jnp.bfloat16)
    )


def fits_fused(n, cfgs, tps, queries, text_keys, frame_counts, out_weight):
    heads = queries.shape[2] // HEAD_DIM
    chips = n // CORES
    if cfgs != 2 or tps != 2 or n % CORES or frame_counts.shape[0] != 1:
        return False
    if chips != 4 or heads % chips or heads // chips < 4:
        return False
    if 3 * queries.shape[1] + 2 * text_keys.shape[1] > n * queries.shape[1]:
        return False
    return out_weight.shape[1] % (8 * HEAD_DIM) == 0 and queries.shape[1] % 16 == 0


def body(n, cfgs, tps, queries, keys, values, text_keys, text_values, prompt_lengths, frame_counts, out_weight):
    rows = queries.shape[1]
    if fits_fused(n, cfgs, tps, queries, text_keys, frame_counts, out_weight):
        return fused_step(
            queries[0], keys[0], values[0], text_keys[0], text_values[0],
            prompt_lengths, frame_counts, out_weight, n,
        )
    attended = gathered_attention(
        queries[0], keys[0], values[0], text_keys[0], text_values[0],
        prompt_lengths, frame_counts, n,
    )
    branch = lax.psum_scatter(
        lax.dot_general(
            out_weight, attended, (((0,), (1,)), ((), ())), preferred_element_type=jnp.float32
        ).astype(jnp.bfloat16),
        "tp",
        scatter_dimension=0,
        tiled=True,
    )
    half = branch.shape[0] // cfgs
    mine = lax.axis_index("cfg")
    kept = lax.dynamic_slice_in_dim(branch, mine * half, half, 0)
    given = lax.dynamic_slice_in_dim(branch, (1 - mine) * half, half, 0)
    other = lax.ppermute(given, "cfg", [(0, 1), (1, 0)])
    first = mine == 0
    conditional = jnp.where(first, kept, other).astype(jnp.float32)
    unconditional = jnp.where(first, other, kept).astype(jnp.float32)
    guided = unconditional + GUIDANCE * (conditional - unconditional)
    valid = (jnp.arange(rows, dtype=jnp.int32) < frame_counts[0])[None, :]

    def local_sum(field):
        return jnp.sum(jnp.where(valid, field, 0.0), axis=1)

    sums = lax.psum(
        jnp.stack([
            local_sum(guided),
            local_sum(guided * guided),
            local_sum(conditional),
            local_sum(conditional * conditional),
            jnp.full((half,), frame_counts[0].astype(jnp.float32)),
        ]),
        "seq",
    )
    means = sums[:4] / sums[4:5]
    guided_mean = means[0]
    guided_var = means[1] - guided_mean * guided_mean
    cond_var = means[3] - means[2] * means[2]
    std_ratio = jnp.sqrt((cond_var + 1.0) / (guided_var + 1.0))
    factor = RESCALE * std_ratio + (1.0 - RESCALE)
    velocity = guided_mean[:, None] + (guided - guided_mean[:, None]) * factor[:, None]
    return velocity.astype(jnp.bfloat16).T


def solution(mesh):
    placed = (
        P("cfg", "seq", "tp"),
        P("cfg", "seq", "tp"),
        P("cfg", "seq", "tp"),
        P("cfg", None, "tp"),
        P("cfg", None, "tp"),
        P("cfg"),
        P("seq"),
        P("tp", None),
    )
    return jax.shard_map(
        functools.partial(body, mesh.shape["seq"], mesh.shape["cfg"], mesh.shape["tp"]),
        mesh=mesh, in_specs=placed, out_specs=P("seq", ("tp", "cfg")), check_vma=False,
    )
```

```python
import functools

import jax
import jax.numpy as jnp
from jax import lax
from jax.experimental import pallas as pl
from jax.experimental.pallas import tpu as pltpu
from jax.sharding import PartitionSpec as P

HEAD_DIM = 128
GUIDANCE = 5.0
RESCALE = 0.7
NEGATIVE = -1e30
LOG2E = 1.4426950408889634
CORES = 2
MESH = pl.DeviceIdType.MESH


def chunk_rows(total, limit):
    for unit in (256, 128, 16):
        for size in range(limit // unit * unit, 0, -unit):
            if total % size == 0:
                return size
    return total


def step_kernel(
    n, chips, group, rows, text, wide, part,
    q, k, v, tk, tv, w, counts, lengths,
    out,
    qb, kb, vb, tkb, tvb, mc, cb, bias, tbias, ob, ab, wb, acc, st, sg, vel,
    send, krecv, qrecv, frecv, count, local, orecv, passed, direct, relayed, wsem, stat, vsem,
):
    me = lax.axis_index("seq")
    t = lax.axis_index("tp")
    c = lax.axis_index("cfg")
    core = lax.rem(me, CORES)
    chip = lax.div(me, CORES)
    partner = chip * CORES + (CORES - 1 - core)
    scale = LOG2E * HEAD_DIM ** (-0.5)
    last = group - 1
    half = chips // 2
    bf16 = jnp.bfloat16
    f32 = jnp.float32

    def cols(owner, head):
        return pl.ds(pl.multiple_of((owner * group + head) * HEAD_DIM, HEAD_DIM), HEAD_DIM)

    def out_cols(side, branch):
        return pl.ds(pl.multiple_of((side * 2 + branch) * wide, HEAD_DIM), wide)

    def slot(index):
        return pl.ds(pl.multiple_of(index * rows, 16), rows)

    def chip_at(step):
        return lax.rem(chip + step, chips)

    mid = chips // 2
    upper = lax.div(chip, mid)
    lower = 1 - upper
    gap = lax.rem(upper * chip + lower * (chips - 1 - chip) + chips + 1 - mid, chips)
    at_end = lax.rem(chip, chips - 1) == 0
    inside = lax.rem(chip, chips - 1) != 0

    def source(place):
        other = lax.rem(mid - 1 + place + lax.div(place + chips - gap, chips), chips)
        other = upper * other + lower * (chips - 1 - other)
        return jnp.where(place == 0, chip, other)

    def turned(step):
        return upper * step + lower * (chips - step)

    def step_from(other):
        return lax.rem(chip + chips - other, chips)

    def step_to(other):
        return lax.rem(other + chips - chip, chips)

    def chip_back(step):
        return lax.rem(chip + chips - step, chips)

    def across(src, dst, sends, recvs, device):
        return pltpu.make_async_remote_copy(
            src_ref=src, dst_ref=dst, send_sem=sends, recv_sem=recvs,
            device_id=device, device_id_type=MESH,
        )

    def drain(ref, sem):
        pltpu.make_async_copy(ref, ref, sem).wait()

    def blocks_of(number):
        return kb.at[0, pl.ds(0, number * rows)]

    x_side = {"tp": 1 - t}
    y_side = {"cfg": 1 - c}

    def kv_copies(head, step):
        target = chip_at(step)
        return [
            across(
                src.at[:, cols(target, head)], dst.at[head, slot(me)],
                send.at[head], krecv.at[head, step - 1], {"seq": target * CORES + core},
            )
            for src, dst in ((k, kb), (v, vb))
        ]

    def q_copy(head, step):
        target = chip_at(step)
        return across(
            q.at[:, cols(target, head)], qb.at[head, chip],
            send.at[head], qrecv.at[head, step - 1], {"seq": target * CORES + core},
        )

    def own_copies(head):
        return [
            pltpu.make_async_copy(k.at[:, cols(chip, head)], kb.at[head, slot(me)], local.at[head]),
            pltpu.make_async_copy(v.at[:, cols(chip, head)], vb.at[head, slot(me)], local.at[head]),
            pltpu.make_async_copy(q.at[:, cols(chip, head)], qb.at[head, chip], local.at[head]),
            pltpu.make_async_copy(tk.at[:, cols(chip, head)], tkb.at[head], local.at[head]),
            pltpu.make_async_copy(tv.at[:, cols(chip, head)], tvb.at[head], local.at[head]),
        ]

    def own_forward(head):
        return [
            across(
                src.at[:, cols(chip, head)], dst.at[head, slot(me)],
                send.at[head], frecv.at[head], {"seq": partner},
            )
            for src, dst in ((k, kb), (v, vb))
        ]

    def forwards(head, step):
        span = slot(chip_back(step) * CORES + core)
        return [
            across(
                buf.at[head, span], buf.at[head, span], send.at[head], frecv.at[head],
                {"seq": partner},
            )
            for buf in (kb, vb)
        ]

    def count_copy(step):
        return across(
            mc, cb.at[me], count.at[0], count.at[1],
            {"seq": lax.rem(me + step, n)},
        )

    def out_copy(head, step):
        target = chip_at(step)
        return across(
            ob.at[head, target], ab.at[c, t, head, chip],
            send.at[head], orecv.at[head, step], {"seq": target * CORES + core},
        )

    def own_out(head):
        return pltpu.make_async_copy(
            ob.at[head, chip], ab.at[c, t, head, chip], orecv.at[head, 0]
        )

    def arrived(head, place, turn):
        if place // half == turn:
            return passed.at[head, place]
        return direct.at[head]

    def x_copy(head, place):
        piece = ab.at[c, t, head, source(place)]
        return across(piece, piece, send.at[head], arrived(head, place, 1), x_side)

    def y_copy(head, place):
        piece = ab.at[c, t, head, source(place)]
        return across(piece, piece, send.at[head], arrived(head, place, 0), y_side)

    def relay(head, place):
        if place < half:
            piece = ab.at[1 - c, t, head, source(place)]
            side = x_side
        else:
            piece = ab.at[c, 1 - t, head, source(place)]
            side = y_side
        return across(piece, piece, send.at[head], relayed.at[head], side)

    def w_own(head):
        return pltpu.make_async_copy(
            w.at[:, head, :, out_cols(t, c)], wb.at[head, t], wsem.at[0]
        )

    def w_copy(head):
        part = pl.ds(core * half, half)
        return across(
            w.at[part, head, :, out_cols(1 - t, c)], wb.at[head, t, part],
            wsem.at[3], wsem.at[1], x_side,
        )

    def w_forward(head):
        place = wb.at[head, 1 - t, pl.ds(core * half, half)]
        return across(place, place, wsem.at[3], wsem.at[2], {"seq": partner})

    parts = wide // part

    def stat_copy(turn, step):
        span = (pl.ds(0, parts - 1), pl.ds(parts - 1, 1))[turn]
        return across(
            st.at[span], sg.at[me, span], stat.at[0], stat.at[1],
            {"seq": lax.rem(me + step, n)},
        )

    mc[...] = jnp.full(mc.shape, counts[0], jnp.int32)
    barrier = pltpu.get_barrier_semaphore()
    for step in range(1, n):
        pl.semaphore_signal(
            barrier, inc=1, device_id={"seq": lax.rem(me + step, n)}, device_id_type=MESH
        )
    pl.semaphore_signal(barrier, inc=1, device_id=x_side, device_id_type=MESH)
    pl.semaphore_signal(barrier, inc=1, device_id=y_side, device_id_type=MESH)

    def start_own(head, _):
        for copy in own_copies(head):
            copy.start()
        w_own(head).start()
        return 0

    lax.fori_loop(0, group, start_own, 0)
    pl.semaphore_wait(barrier, n + 1)

    def start_kv(head):
        for step in range(1, chips):
            for copy in kv_copies(head, turned(step)):
                copy.start()

    def start_q(head):
        for step in range(1, chips):
            q_copy(head, turned(step)).start()

    for step in range(1, n):
        count_copy(step).start()
    start_kv(0)
    start_q(0)

    @pl.when(inside)
    def _():
        start_kv(1)


    def start_near(head, _):
        w_copy(head).start()
        for copy in own_forward(head):
            copy.start()
        return 0

    lax.fori_loop(0, group, start_near, 0)

    cb[me] = mc[...]
    st[...] = jnp.zeros_like(st)
    acc[...] = jnp.zeros_like(acc)
    drain(cb.at[pl.ds(0, n - 1)], count.at[1])
    lane = lax.broadcasted_iota(jnp.int32, (rows, HEAD_DIM), 1)
    place_in = lax.broadcasted_iota(jnp.int32, (rows, HEAD_DIM), 0)

    def fill_bias(origin, _):
        limit = cb[origin][0:1, :]
        bias[slot(origin), :] = jnp.where(
            (lane == 0) & (place_in >= limit), NEGATIVE, 0.0
        ).astype(bf16)
        return 0

    lax.fori_loop(0, n, fill_bias, 0)
    tlane = lax.broadcasted_iota(jnp.int32, (text, HEAD_DIM), 1)
    tplace = lax.broadcasted_iota(jnp.int32, (text, HEAD_DIM), 0)
    tbias[...] = jnp.where(
        (tlane == 0) & (tplace >= lengths[0]), NEGATIVE, 0.0
    ).astype(bf16)

    total = n * rows
    size = chunk_rows(total, 768)

    def ones(length):
        return jnp.where(
            lax.broadcasted_iota(jnp.int32, (length, HEAD_DIM), 1) == 0, 1.0, 0.0
        ).astype(bf16)

    def one_block(head, target):
        query = jnp.concatenate([qb[head, target], ones(rows)], axis=1)

        def piece(state, keys, masks, vals):
            keys = jnp.concatenate([keys, masks], axis=1)
            vals = jnp.concatenate([vals, ones(vals.shape[0])], axis=1)
            scores = lax.dot_general(
                query, keys, (((1,), (1,)), ((), ())), preferred_element_type=f32
            )
            high = jnp.max(scores, axis=1, keepdims=True) * scale
            if state is not None:
                high = jnp.maximum(high, state[0])
            weights = jnp.exp2(scores * scale - high).astype(bf16)
            mixed = jnp.dot(weights, vals, preferred_element_type=f32)
            if state is not None:
                mixed = mixed + state[1] * jnp.exp2(state[0] - high)
            return (high, mixed)

        state = piece(None, tkb[head], tbias[...], tvb[head])
        for start in range(0, total, size):
            span = pl.ds(start, size)
            state = piece(state, kb[head, span], bias[span, :], vb[head, span])
        mixed = state[1]
        ob[head, target] = (
            mixed[:, :HEAD_DIM] / mixed[:, HEAD_DIM:HEAD_DIM + 1]
        ).astype(bf16)

    def take_keys(head):
        drain(kb.at[0, pl.ds(0, 3 * rows + 2 * text)], local.at[head])
        for step in range(1, chips):
            drain(blocks_of(2), krecv.at[head, turned(step) - 1])
            for copy in forwards(head, turned(step)):
                copy.start()
        drain(blocks_of(n), frecv.at[head])

    def share_piece(head, place):
        if place == 0:
            own_out(head).wait()
        else:
            out_copy(head, step_from(source(place))).wait_recv()
        x_copy(head, place).start()
        y_copy(head, place).start()

    def share(head, places):
        for place in places:
            share_piece(head, place)

    def pass_on(head, places):
        for place in places:
            drain(blocks_of(1), passed.at[head, place])
            relay(head, place).start()

    def blocks(head, after):
        def block(place, _):
            other = source(place)
            far = place > 0

            @pl.when(far)
            def _():
                q_copy(head, step_from(other)).wait_recv()

            if after is None:
                @pl.when((place == chips - 1) & at_end)
                def _():
                    start_kv(head + 1)

            one_block(head, other)

            @pl.when(far)
            def _():
                out_copy(head, step_to(other)).start()

            @pl.when(place == 0)
            def _():
                own_out(head).start()
                share_piece(head, 0)

            if after is not None:
                after(place)
            return 0

        lax.fori_loop(0, chips, block, 0)

    def collect_direct(head):
        drain(blocks_of(chips), direct.at[head])

    def collect_relayed(head):
        drain(blocks_of(chips), relayed.at[head])

    def collect(head):
        collect_direct(head)
        collect_relayed(head)

    depth = 2 * chips * HEAD_DIM

    def product(head, branch, span):
        rows_in = jnp.concatenate(
            [ab[branch, side, head, owner] for side in range(2) for owner in range(chips)],
            axis=1,
        )
        weight = wb[head, :, :, :, span].reshape(depth, part)
        return jnp.dot(rows_in, weight, preferred_element_type=f32)

    def side_product(head, branch, side, span):
        rows_in = jnp.concatenate(
            [ab[branch, side, head, owner] for owner in range(chips)], axis=1
        )
        weight = wb[head, side, :, :, span].reshape(chips * HEAD_DIM, part)
        return jnp.dot(rows_in, weight, preferred_element_type=f32)

    def span_of(index):
        return pl.ds(pl.multiple_of(index * part, HEAD_DIM), part)

    def project(head):
        def one(index, _):
            span = span_of(index)
            for branch in range(2):
                acc[branch, :, span] += product(head, branch, span)
            return 0

        lax.fori_loop(0, parts, one, 0)

    def project_branch(head, branch):
        def one(index, _):
            span = span_of(index)
            acc[branch, :, span] += product(head, branch, span)
            return 0

        lax.fori_loop(0, parts, one, 0)

    def project_side(head, branch, side):
        def one(index, _):
            span = span_of(index)
            acc[branch, :, span] += side_product(head, branch, side, span)
            return 0

        lax.fori_loop(0, parts, one, 0)

    near = pl.ds(0, half)

    def pass_weight(index, _):
        w_forward(index).start()
        return 0

    def one_head(head, _):
        take_keys(head)
        blocks(head, None)
        start_q(head + 1)

        @pl.when(inside & (head + 2 <= last))
        def _():
            start_kv(head + 2)

        @pl.when(head == 1)
        def _():
            drain(wb.at[:, 0, near], wsem.at[1])
            lax.fori_loop(0, group, pass_weight, 0)

        @pl.when(head >= 1)
        def _():
            share(head - 1, range(1, chips))

        @pl.when(head == 2)
        def _():
            drain(wb.at[:, 0], wsem.at[0])
            drain(wb.at[:, 0, near], wsem.at[2])

        @pl.when(head >= 2)
        def _():
            collect(head - 2)
            project(head - 2)

        @pl.when(head >= 1)
        def _():
            pass_on(head - 1, range(chips))

        return 0

    lax.fori_loop(0, last, one_head, 0)
    early = range(1, chips - 1)
    collect(last - 2)
    project(last - 2)
    share(last - 1, early)

    take_keys(last)

    def after_block(place):
        @pl.when(place == 0)
        def _():
            share_piece(last - 1, chips - 1)

        @pl.when(place == 1)
        def _():
            pass_on(last - 1, range(chips - 1))

        @pl.when(place == chips - 2)
        def _():
            pass_on(last - 1, (chips - 1,))
            pass_on(last, (0,))

    blocks(last, after_block)
    share(last, early)
    collect(last - 1)
    project(last - 1)
    share(last, (chips - 1,))
    pass_on(last, range(1, chips))
    collect_direct(last)
    project_branch(last, c)
    project_side(last, 1 - c, t)
    collect_relayed(last)

    limit = cb[me][0:1, 0:1]
    valid = lax.broadcasted_iota(jnp.int32, (rows, part), 0) < limit
    first = jnp.full((rows, part), c, jnp.int32) == 0
    pairs = part // HEAD_DIM

    def guide(index):
        span = pl.ds(index * part, part)
        mine = acc[c, :, span].astype(bf16).astype(f32)
        other = acc[1 - c, :, span] + side_product(last, 1 - c, 1 - t, span)
        other = other.astype(bf16).astype(f32)
        conditional = jnp.where(first, mine, other)
        unconditional = jnp.where(first, other, mine)
        guided = unconditional + GUIDANCE * (conditional - unconditional)
        acc[0, :, span] = guided
        guided = jnp.where(valid, guided, 0.0)
        conditional = jnp.where(valid, conditional, 0.0)
        for row, field in enumerate(
            (guided, guided * guided, conditional, conditional * conditional)
        ):
            total_row = jnp.sum(field, axis=0, keepdims=True)
            for pair in range(pairs):
                st[index, 4 * pair + row:4 * pair + row + 1, :] = total_row[
                    :, pair * HEAD_DIM:(pair + 1) * HEAD_DIM
                ]

    for index in range(parts):
        guide(index)
        if index >= parts - 2:
            for step in range(1, n):
                stat_copy(index + 2 - parts, step).start()

    def settle(head, _):
        drain(kb.at[pl.ds(0, chips)], send.at[head])
        return 0

    lax.fori_loop(0, group, settle, 0)
    drain(wb.at[:, 0], wsem.at[3])
    drain(cb.at[pl.ds(0, n - 1)], count.at[0])
    valid_total = cb[0][0:1, :]
    for origin in range(1, n):
        valid_total = valid_total + cb[origin][0:1, :]
    valid_total = valid_total.astype(f32)

    def store(index):
        return pltpu.make_async_copy(vel.at[index], out.at[:, span_of(index)], vsem.at[0])

    drain(sg.at[pl.ds(0, n - 1)], stat.at[1])

    def finish(index, _):
        sums = st[index]
        for step in range(1, n):
            sums = sums + sg[lax.rem(me + step, n), index]
        for pair in range(pairs):
            here = sums[4 * pair:4 * pair + 4] / valid_total
            guided_mean = here[0:1, :]
            guided_var = here[1:2, :] - guided_mean * guided_mean
            cond_mean = here[2:3, :]
            cond_var = here[3:4, :] - cond_mean * cond_mean
            std_ratio = jnp.sqrt((cond_var + 1.0) / (guided_var + 1.0))
            factor = RESCALE * std_ratio + (1.0 - RESCALE)
            span = pl.ds(pl.multiple_of(index * part + pair * HEAD_DIM, HEAD_DIM), HEAD_DIM)
            vel[index, :, pair * HEAD_DIM:(pair + 1) * HEAD_DIM] = (
                guided_mean + (acc[0, :, span] - guided_mean) * factor
            ).astype(bf16)
        store(index).start()
        return 0

    lax.fori_loop(0, parts, finish, 0)

    drain(sg.at[pl.ds(0, n - 1)], stat.at[0])
    drain(vel, vsem.at[0])


def fused_step(
    queries, keys, values, text_keys, text_values, prompt_lengths, frame_counts, out_weight, n
):
    rows, width = queries.shape
    text = text_keys.shape[0]
    chips = n // CORES
    heads = width // HEAD_DIM
    group = heads // chips
    wide = out_weight.shape[1] // 4
    part = 256 if wide % 256 == 0 else HEAD_DIM
    parts = wide // part
    weight = out_weight.reshape(chips, group, HEAD_DIM, out_weight.shape[1])
    bf16 = jnp.bfloat16
    f32 = jnp.float32
    total = n * rows
    hbm = pl.BlockSpec(memory_space=pl.ANY)
    smem = pl.BlockSpec(memory_space=pltpu.SMEM)
    dma = pltpu.SemaphoreType.DMA
    return pl.pallas_call(
        functools.partial(step_kernel, n, chips, group, rows, text, wide, part),
        out_shape=jax.ShapeDtypeStruct((rows, wide), bf16),
        in_specs=[hbm] * 6 + [smem] * 2,
        out_specs=hbm,
        scratch_shapes=[
            pltpu.VMEM((group, chips, rows, HEAD_DIM), bf16),
            pltpu.VMEM((group, total, HEAD_DIM), bf16),
            pltpu.VMEM((group, total, HEAD_DIM), bf16),
            pltpu.VMEM((group, text, HEAD_DIM), bf16),
            pltpu.VMEM((group, text, HEAD_DIM), bf16),
            pltpu.VMEM((8, HEAD_DIM), jnp.int32),
            pltpu.VMEM((n, 8, HEAD_DIM), jnp.int32),
            pltpu.VMEM((total, HEAD_DIM), bf16),
            pltpu.VMEM((text, HEAD_DIM), bf16),
            pltpu.VMEM((group, chips, rows, HEAD_DIM), bf16),
            pltpu.VMEM((2, 2, group, chips, rows, HEAD_DIM), bf16),
            pltpu.VMEM((group, 2, chips, HEAD_DIM, wide), bf16),
            pltpu.VMEM((2, rows, wide), f32),
            pltpu.VMEM((parts, 8, HEAD_DIM), f32),
            pltpu.VMEM((n, parts, 8, HEAD_DIM), f32),
            pltpu.VMEM((parts, rows, part), bf16),
            dma((group,)),
            dma((group, chips - 1)),
            dma((group, chips - 1)),
            dma((group,)),
            dma((2,)),
            dma((group,)),
            dma((group, chips)),
            dma((group, chips)),
            dma((group,)),
            dma((group,)),
            dma((4,)),
            dma((2,)),
            dma((1,)),
        ],
        compiler_params=pltpu.CompilerParams(
            collective_id=0, has_side_effects=True, vmem_limit_bytes=52 * 1024 * 1024
        ),
    )(queries, keys, values, text_keys, text_values, weight, frame_counts, prompt_lengths)


def frame_valid(positions, counts_table, slots):
    frame_index = positions // slots
    slot_index = positions % slots
    frame_ids = jnp.arange(counts_table.shape[0], dtype=jnp.int32)
    frame_limit = jnp.sum(
        jnp.where(frame_index[:, None] == frame_ids[None, :], counts_table[None, :], 0), axis=1
    )
    return slot_index < frame_limit


def attend_block(carry, key_rows, value_rows, query_heads, key_mask):
    row_max, weight_sum, mixed_sum = carry
    head_count = query_heads.shape[1]
    key_heads = key_rows.reshape(key_rows.shape[0], head_count, HEAD_DIM)
    value_heads = value_rows.reshape(value_rows.shape[0], head_count, HEAD_DIM)
    scores = jnp.einsum(
        "qhd,khd->hqk", query_heads, key_heads, preferred_element_type=jnp.float32
    ) * HEAD_DIM ** (-0.5)
    scores = jnp.where(key_mask[None, None, :], scores, NEGATIVE)
    new_max = jnp.maximum(row_max, jnp.max(scores, axis=2))
    shrink = jnp.exp(row_max - new_max)
    weights = jnp.exp(scores - new_max[:, :, None])
    weight_sum = weight_sum * shrink + jnp.sum(weights, axis=2)
    mixed_sum = mixed_sum * shrink[:, :, None] + jnp.einsum(
        "hqk,khd->hqd",
        weights.astype(jnp.bfloat16),
        value_heads,
        preferred_element_type=jnp.float32,
    )
    return (new_max, weight_sum, mixed_sum)


def gathered_attention(
    queries, keys, values, text_keys, text_values, prompt_lengths, frame_counts, n
):
    row_count, head_cols = queries.shape
    head_count = head_cols // HEAD_DIM
    all_counts = lax.all_gather(frame_counts, "seq", axis=0, tiled=True)
    query_heads = queries.reshape(row_count, head_count, HEAD_DIM)
    text_mask = jnp.arange(text_keys.shape[0], dtype=jnp.int32) < prompt_lengths[0]
    empty_state = (
        jnp.full((head_count, row_count), NEGATIVE, jnp.float32),
        jnp.zeros((head_count, row_count), jnp.float32),
        jnp.zeros((head_count, row_count, HEAD_DIM), jnp.float32),
    )
    text_state = attend_block(empty_state, text_keys, text_values, query_heads, text_mask)
    key_rows = lax.all_gather(keys, "seq", axis=0, tiled=True)
    value_rows = lax.all_gather(values, "seq", axis=0, tiled=True)
    positions = jnp.arange(key_rows.shape[0], dtype=jnp.int32)
    _, weight_sum, mixed_sum = attend_block(
        text_state, key_rows, value_rows, query_heads,
        frame_valid(positions, all_counts, row_count // frame_counts.shape[0]),
    )
    return (
        jnp.transpose(mixed_sum / weight_sum[:, :, None], (1, 0, 2))
        .reshape(row_count, head_cols)
        .astype(jnp.bfloat16)
    )


def fits_fused(n, cfgs, tps, queries, text_keys, frame_counts, out_weight):
    heads = queries.shape[2] // HEAD_DIM
    chips = n // CORES
    if cfgs != 2 or tps != 2 or n % CORES or frame_counts.shape[0] != 1:
        return False
    if chips != 4 or heads % chips or heads // chips < 4:
        return False
    if 3 * queries.shape[1] + 2 * text_keys.shape[1] > n * queries.shape[1]:
        return False
    return out_weight.shape[1] % (8 * HEAD_DIM) == 0 and queries.shape[1] % 16 == 0


def body(n, cfgs, tps, queries, keys, values, text_keys, text_values, prompt_lengths, frame_counts, out_weight):
    rows = queries.shape[1]
    if fits_fused(n, cfgs, tps, queries, text_keys, frame_counts, out_weight):
        return fused_step(
            queries[0], keys[0], values[0], text_keys[0], text_values[0],
            prompt_lengths, frame_counts, out_weight, n,
        )
    attended = gathered_attention(
        queries[0], keys[0], values[0], text_keys[0], text_values[0],
        prompt_lengths, frame_counts, n,
    )
    branch = lax.psum_scatter(
        lax.dot_general(
            out_weight, attended, (((0,), (1,)), ((), ())), preferred_element_type=jnp.float32
        ).astype(jnp.bfloat16),
        "tp",
        scatter_dimension=0,
        tiled=True,
    )
    half = branch.shape[0] // cfgs
    mine = lax.axis_index("cfg")
    kept = lax.dynamic_slice_in_dim(branch, mine * half, half, 0)
    given = lax.dynamic_slice_in_dim(branch, (1 - mine) * half, half, 0)
    other = lax.ppermute(given, "cfg", [(0, 1), (1, 0)])
    first = mine == 0
    conditional = jnp.where(first, kept, other).astype(jnp.float32)
    unconditional = jnp.where(first, other, kept).astype(jnp.float32)
    guided = unconditional + GUIDANCE * (conditional - unconditional)
    valid = (jnp.arange(rows, dtype=jnp.int32) < frame_counts[0])[None, :]

    def local_sum(field):
        return jnp.sum(jnp.where(valid, field, 0.0), axis=1)

    sums = lax.psum(
        jnp.stack([
            local_sum(guided),
            local_sum(guided * guided),
            local_sum(conditional),
            local_sum(conditional * conditional),
            jnp.full((half,), frame_counts[0].astype(jnp.float32)),
        ]),
        "seq",
    )
    means = sums[:4] / sums[4:5]
    guided_mean = means[0]
    guided_var = means[1] - guided_mean * guided_mean
    cond_var = means[3] - means[2] * means[2]
    std_ratio = jnp.sqrt((cond_var + 1.0) / (guided_var + 1.0))
    factor = RESCALE * std_ratio + (1.0 - RESCALE)
    velocity = guided_mean[:, None] + (guided - guided_mean[:, None]) * factor[:, None]
    return velocity.astype(jnp.bfloat16).T


def solution(mesh):
    placed = (
        P("cfg", "seq", "tp"),
        P("cfg", "seq", "tp"),
        P("cfg", "seq", "tp"),
        P("cfg", None, "tp"),
        P("cfg", None, "tp"),
        P("cfg"),
        P("seq"),
        P("tp", None),
    )
    return jax.shard_map(
        functools.partial(body, mesh.shape["seq"], mesh.shape["cfg"], mesh.shape["tp"]),
        mesh=mesh, in_specs=placed, out_specs=P("seq", ("tp", "cfg")), check_vma=False,
    )
```
